128 devices in a mesh: dev: 128 (over x, z, y, core).
Axes of the slice: x: 4, y: 4, z: 4, core: 2. Of those that a mesh axis runs over, the one named last changes fastest.
Arguments:
- pixels: float32 [4, 2048, 8192], P(None, 'dev'), may hold values from -10 to 10
- valid_flags: int32 [4, 2048, 8192], P(None, 'dev'), may hold values 0 or 1
Outputs:
- tile_halves: float32 [128, 256, 2048], P('dev')
- header: float32 [5, 4], replicated
The draws below stay inside these ranges and needn't reach their ends.
All inputs are finite; a program needn't handle non-finite values. No bound on the sum of `valid_flags` on one device may be relied on, other than what follows from the above.
Results may differ from the reference program's by a relative error of at most 0.00002.
Values sent between devices are 32-bit elements; how exact they have to be, the bound alone decides.
A program may use at most 128 MiB of HBM per device.

```python
import jax
import jax.numpy as jnp
from jax import lax

BANDS = 4
TILE = 512
STRIP = 16
GROUP = 16
COLS = 8192
ROWS = 2048
HALF = 256
N_DEV = 128


def draw_pixels(key, part):
    first_key, second_key, third_key = jax.random.split(jax.random.fold_in(key, 11), 3)
    strip_count = ROWS // STRIP
    offsets = jax.random.uniform(first_key, (BANDS, strip_count, 1, 1), jnp.float32, -2.0, 2.0)
    widths = jnp.exp(jax.random.uniform(second_key, (BANDS, strip_count, 1, 1), jnp.float32, jnp.log(0.5), jnp.log(2.0)))
    noise = jnp.clip(jax.random.normal(third_key, (BANDS, strip_count, STRIP, COLS), jnp.float32), -4.0, 4.0)
    values = offsets + widths * noise
    return values.reshape(BANDS, ROWS, COLS).astype(jnp.float32)


def set_ends(result, own_key, low, high):
    longest = result.shape.index(max(result.shape))
    spots = []
    for shift in (0, 1):
        where = [jax.random.randint(jax.random.fold_in(own_key, axis), (), 0, length) for axis, length in enumerate(result.shape)]
        where[longest] = (where[longest] + shift) % result.shape[longest]
        spots.append(tuple(where))
    return result.at[spots[0]].set(low).at[spots[1]].set(high)


def setup_inputs(seed: int = 0) -> dict:
    streams_of = jax.random.split(jax.random.key(seed), 3)
    pixels = draw_pixels(jax.random.fold_in(streams_of[2], 71), 0)
    valid_flags = set_ends((jax.random.randint(streams_of[1], (BANDS, ROWS, COLS), 0, 4) < 3).astype(jnp.int32), jax.random.fold_in(streams_of[1], 1), 0, 1)
    return dict(pixels=pixels, valid_flags=valid_flags)


largest_value = 3e+38

def reference(pixels, valid_flags):
    usable = valid_flags == 1
    filled = jnp.where(usable, pixels, jnp.float32(0.0))
    blocks = filled.reshape(BANDS, ROWS // HALF, HALF, GROUP, TILE)
    tile_halves = jnp.transpose(blocks, (1, 3, 2, 4, 0)).reshape(N_DEV, HALF, TILE * BANDS)
    lowest = lax.optimization_barrier(jnp.min(jnp.where(usable, pixels, jnp.float32(largest_value)), axis=(1, 2)))
    highest = lax.optimization_barrier(jnp.max(jnp.where(usable, pixels, jnp.float32(-largest_value)), axis=(1, 2)))
    valid_count = lax.optimization_barrier(jnp.sum(usable.astype(jnp.float32), axis=(1, 2)))
    band_sum = lax.optimization_barrier(jnp.sum(filled, axis=(1, 2)))
    band_squares = lax.optimization_barrier(jnp.sum(filled * filled, axis=(1, 2)))
    divisor = jnp.maximum(valid_count, 1.0)
    average = band_sum / divisor
    variance = band_squares / divisor - average * average
    header = jnp.stack([lowest, highest, valid_count / (ROWS * COLS), average, jnp.sqrt(jnp.maximum(variance, 0.25))])
    return (tile_halves, header)
```

```python
import jax
import jax.numpy as jnp
from jax import lax
from jax.experimental import pallas as pl
from jax.experimental.pallas import tpu as pltpu
from jax.sharding import PartitionSpec as P

BANDS = 4
TILE = 512
STRIP = 16
GROUP = 16
HALF = 256
N_DEV = 128
WIDE = TILE * BANDS
CELLS = 16777216.0
LARGEST = 3e38
LANES = 128


def partner(pos, i):
    dy = 3 - i % 4
    dc = 1 - (i // 4) % 2
    dz = 1 - i // 8
    z, y, c = pos // 8, (pos // 2) % 4, pos % 2
    return ((z + dz) % 2) * 8 + ((y + dy) % 4) * 2 + (c + dc) % 2


def far_partner(me, k):
    group, pos = me // GROUP, me % GROUP
    return ((group + k) % 8) * GROUP + pos


def merge(a, b, row):
    return jnp.where(row == 0, jnp.minimum(a, b), jnp.where(row == 1, jnp.maximum(a, b), a + b))


def kernel(px_hbm, fl_hbm, out, header, px, fl, send, stat_own, stat_in, group_own, group_in,
           in_sem, send_sem, recv_sem, s1_send, s1_recv, s2_send, s2_recv):
    me = lax.axis_index("dev")
    base = (me // GROUP) * GROUP
    pos = me % GROUP

    def load_px(i):
        at = pl.multiple_of(partner(pos, i) * TILE, TILE)
        return pltpu.make_async_copy(px_hbm.at[:, :, pl.ds(at, TILE)], px.at[i], in_sem.at[0, i])

    def load_fl(i):
        at = pl.multiple_of(partner(pos, i) * TILE, TILE)
        return pltpu.make_async_copy(fl_hbm.at[:, :, pl.ds(at, TILE)], fl.at[i], in_sem.at[1, i])

    def start_load(i, _):
        load_px(i).start()
        load_fl(i).start()
        return 0

    lax.fori_loop(0, GROUP, start_load, 0)

    barrier = pltpu.get_barrier_semaphore()

    def greet(i, _):
        pl.semaphore_signal(barrier, inc=1, device_id=(base + partner(pos, i),),
                            device_id_type=pl.DeviceIdType.MESH)
        return 0

    def greet_far(k, _):
        pl.semaphore_signal(barrier, inc=1, device_id=(far_partner(me, k),),
                            device_id_type=pl.DeviceIdType.MESH)
        return 0

    lax.fori_loop(0, 15, greet, 0)
    lax.fori_loop(1, 8, greet_far, 0)

    my_rows = pl.multiple_of(pos * STRIP, STRIP)

    def piece(i):
        return pltpu.make_async_remote_copy(
            src_ref=send.at[i], dst_ref=out.at[pl.ds(my_rows, STRIP)],
            send_sem=send_sem.at[i], recv_sem=recv_sem.at[i],
            device_id=(base + partner(pos, i),), device_id_type=pl.DeviceIdType.MESH)

    def stat_copy(i):
        return pltpu.make_async_remote_copy(
            src_ref=stat_own, dst_ref=stat_in.at[i],
            send_sem=s1_send.at[i], recv_sem=s1_recv.at[i],
            device_id=(base + partner(pos, i),), device_id_type=pl.DeviceIdType.MESH)

    def group_copy(k):
        return pltpu.make_async_remote_copy(
            src_ref=group_own, dst_ref=group_in.at[k],
            send_sem=s2_send.at[k], recv_sem=s2_recv.at[k],
            device_id=(far_partner(me, k),), device_id_type=pl.DeviceIdType.MESH)

    lane = lax.broadcasted_iota(jnp.int32, (8, LANES), 1)
    row = lax.broadcasted_iota(jnp.int32, (8, LANES), 0)
    block = lane // 32
    order = [((q + lane % 4) % 4) * 32 + lane // 4 for q in range(4)]

    def work(i, carry, store):
        load_px(i).wait()
        load_fl(i).wait()
        low, high, count, total, square = carry
        low, high, count, total, square = list(low), list(high), list(count), list(total), list(square)
        sums = [[] for _ in range(BANDS)]
        squares = [[] for _ in range(BANDS)]
        for r in range(2):
            for j in range(4):
                turned = []
                for b in range(BANDS):
                    value = px[i, b, pl.ds(8 * r, 8), pl.ds(LANES * j, LANES)]
                    flag = fl[i, b, pl.ds(8 * r, 8), pl.ds(LANES * j, LANES)]
                    usable = flag == 1
                    filled = jnp.where(usable, value, 0.0)
                    low[b] = jnp.minimum(low[b], jnp.where(usable, value, LARGEST))
                    high[b] = jnp.maximum(high[b], jnp.where(usable, value, -LARGEST))
                    count[b] = count[b] + flag
                    sums[b].append(filled)
                    squares[b].append(filled * filled)
                    turned.append(filled if b == 0 else pltpu.roll(filled, 32 * b, 1))
                for q in range(4):
                    mixed = turned[(0 - q) % 4]
                    for k in range(1, 4):
                        mixed = jnp.where(block == k, turned[(k - q) % 4], mixed)
                    store(r, j * 4 + q, jnp.take_along_axis(mixed, order[q], axis=1))

        def tree(parts):
            while len(parts) > 1:
                parts = [a + b for a, b in zip(parts[::2], parts[1::2])]
            return parts[0]

        for b in range(BANDS):
            total[b] = total[b] + tree(sums[b])
            square[b] = square[b] + tree(squares[b])
        return (tuple(low), tuple(high), tuple(count), tuple(total), tuple(square))

    zero = jnp.zeros((8, LANES), jnp.float32)
    carry = (
        (zero + LARGEST,) * BANDS, (zero - LARGEST,) * BANDS,
        (jnp.zeros((8, LANES), jnp.int32),) * BANDS, (zero,) * BANDS, (zero,) * BANDS,
    )

    def step(i, carry):
        def store(r, c, value):
            send[i, pl.ds(8 * r, 8), pl.ds(LANES * c, LANES)] = value

        carry = work(i, carry, store)

        @pl.when(i == 0)
        def _():
            pl.semaphore_wait(barrier, 22)

        piece(i).start()
        return carry

    carry = lax.fori_loop(0, 15, step, carry)

    def store_own(r, c, value):
        out[pl.ds(pl.multiple_of(my_rows + 8 * r, 8), 8), pl.ds(LANES * c, LANES)] = value

    low, high, count, total, square = work(15, carry, store_own)

    stats = jnp.zeros((8, LANES), jnp.float32)
    for b in range(BANDS):
        for s, value in enumerate((
            jnp.min(low[b], axis=(0, 1), keepdims=True),
            jnp.max(high[b], axis=(0, 1), keepdims=True),
            jnp.sum(count[b].astype(jnp.float32), axis=(0, 1), keepdims=True),
            jnp.sum(total[b], axis=(0, 1), keepdims=True),
            jnp.sum(square[b], axis=(0, 1), keepdims=True),
        )):
            stats = jnp.where((row == s) & (lane == b), value, stats)
    stat_own[...] = stats

    def start_stat(i, _):
        stat_copy(i).start()
        return 0

    lax.fori_loop(0, 15, start_stat, 0)

    def take_stat(i, acc):
        stat_copy(i).wait_recv()
        return merge(acc, stat_in[i], row)

    acc = lax.fori_loop(0, 15, take_stat, stat_own[...])
    group_own[...] = acc

    def start_group(k, _):
        group_copy(k).start()
        return 0

    lax.fori_loop(1, 8, start_group, 0)

    def take_group(k, acc):
        group_copy(k).wait_recv()
        return merge(acc, group_in[k], row)

    acc = lax.fori_loop(1, 8, take_group, acc)
    valid = acc[2:3]
    divisor = jnp.maximum(valid, 1.0)
    average = acc[3:4] / divisor
    variance = acc[4:5] / divisor - average * average
    header[0:1, :] = acc[0:1, :BANDS]
    header[1:2, :] = acc[1:2, :BANDS]
    header[2:3, :] = (valid / CELLS)[:, :BANDS]
    header[3:4, :] = average[:, :BANDS]
    header[4:5, :] = jnp.sqrt(jnp.maximum(variance, 0.25))[:, :BANDS]

    def finish(i, _):
        piece(i).wait_send()
        piece(i).wait_recv()
        stat_copy(i).wait_send()
        return 0

    lax.fori_loop(0, 15, finish, 0)

    def finish_far(k, _):
        group_copy(k).wait_send()
        return 0

    lax.fori_loop(1, 8, finish_far, 0)


def on_device(pixels, valid_flags):
    dma = pltpu.SemaphoreType.DMA
    tile, header = pl.pallas_call(
        kernel,
        out_shape=(
            jax.ShapeDtypeStruct((HALF, WIDE), jnp.float32),
            jax.ShapeDtypeStruct((5, BANDS), jnp.float32),
        ),
        in_specs=[pl.BlockSpec(memory_space=pl.ANY)] * 2,
        out_specs=(pl.BlockSpec(memory_space=pltpu.VMEM), pl.BlockSpec(memory_space=pltpu.VMEM)),
        scratch_shapes=[
            pltpu.VMEM((GROUP, BANDS, STRIP, TILE), jnp.float32),
            pltpu.VMEM((GROUP, BANDS, STRIP, TILE), jnp.int32),
            pltpu.VMEM((GROUP - 1, STRIP, WIDE), jnp.float32),
            pltpu.VMEM((8, LANES), jnp.float32),
            pltpu.VMEM((GROUP - 1, 8, LANES), jnp.float32),
            pltpu.VMEM((8, LANES), jnp.float32),
            pltpu.VMEM((8, 8, LANES), jnp.float32),
            dma((2, GROUP)), dma((GROUP - 1,)), dma((GROUP - 1,)),
            dma((GROUP - 1,)), dma((GROUP - 1,)), dma((8,)), dma((8,)),
        ],
        compiler_params=pltpu.CompilerParams(collective_id=0, has_side_effects=True),
        name="export",
    )(pixels, valid_flags)
    return tile.reshape(1, HALF, WIDE), header


def solution(mesh):
    placed = (P(None, "dev", None), P(None, "dev", None))
    return jax.shard_map(
        on_device, mesh=mesh, in_specs=placed, out_specs=(P("dev", None, None), P()), check_vma=False
    )
```

```python
import jax
import jax.numpy as jnp
from jax import lax
from jax.experimental import pallas as pl
from jax.experimental.pallas import tpu as pltpu
from jax.sharding import PartitionSpec as P

BANDS = 4
TILE = 512
STRIP = 16
GROUP = 16
HALF = 256
N_DEV = 128
WIDE = TILE * BANDS
CELLS = 16777216.0
LARGEST = 3e38
LANES = 128
EARLY = 10


STEPS = (
    (1, 0, 0), (0, 2, 0), (1, 0, 1), (0, 2, 1), (1, 1, 0), (0, 3, 0), (1, 3, 0), (0, 1, 0),
    (1, 1, 1), (0, 3, 1), (1, 3, 1), (0, 1, 1), (1, 2, 0), (1, 2, 1), (0, 0, 1), (0, 0, 0),
)
CODES = [sum((z * 8 + y * 2 + c) << (4 * k) for k, (z, y, c) in enumerate(STEPS[at:at + 7])) for at in (0, 7, 14)]


def partner(pos, i):
    code = jnp.where(i < 7, CODES[0], jnp.where(i < 14, CODES[1], CODES[2]))
    code = (code >> (4 * (i % 7))) % 16
    dz, dy, dc = code // 8, (code // 2) % 4, code % 2
    z, y, c = pos // 8, (pos // 2) % 4, pos % 2
    return ((z + dz) % 2) * 8 + ((y + dy) % 4) * 2 + (c + dc) % 2


def far_partner(me, k):
    group, pos = me // GROUP, me % GROUP
    return ((group + k) % 8) * GROUP + pos


def merge(a, b, lane):
    return jnp.where(lane == 0, jnp.minimum(a, b), jnp.where(lane == 1, jnp.maximum(a, b), a + b))


def kernel(px_hbm, fl_hbm, out, header, px, fl, send, stat_own, stat_in, group_own, group_in,
           in_sem, send_sem, recv_sem, s1_send, s1_recv, s2_send, s2_recv):
    me = lax.axis_index("dev")
    base = (me // GROUP) * GROUP
    pos = me % GROUP

    def load_px(i):
        at = pl.multiple_of(partner(pos, i) * TILE, TILE)
        return pltpu.make_async_copy(px_hbm.at[:, :, pl.ds(at, TILE)], px.at[i], in_sem.at[0, i])

    def load_fl(i):
        at = pl.multiple_of(partner(pos, i) * TILE, TILE)
        return pltpu.make_async_copy(fl_hbm.at[:, :, pl.ds(at, TILE)], fl.at[i], in_sem.at[1, i])

    def start_load(i, _):
        load_px(i).start()
        load_fl(i).start()
        return 0

    lax.fori_loop(0, GROUP, start_load, 0)

    barrier = pltpu.get_barrier_semaphore()

    def greet(i, _):
        pl.semaphore_signal(barrier, inc=1, device_id=(base + partner(pos, i),),
                            device_id_type=pl.DeviceIdType.MESH)
        return 0

    def greet_far(k, _):
        pl.semaphore_signal(barrier, inc=1, device_id=(far_partner(me, k),),
                            device_id_type=pl.DeviceIdType.MESH)
        return 0

    lax.fori_loop(0, 15, greet, 0)
    lax.fori_loop(1, 8, greet_far, 0)

    my_rows = pl.multiple_of(pos * STRIP, STRIP)

    def piece(i):
        return pltpu.make_async_remote_copy(
            src_ref=send.at[i], dst_ref=out.at[pl.ds(my_rows, STRIP)],
            send_sem=send_sem.at[i], recv_sem=recv_sem.at[i],
            device_id=(base + partner(pos, i),), device_id_type=pl.DeviceIdType.MESH)

    def stat_copy(i):
        return pltpu.make_async_remote_copy(
            src_ref=stat_own, dst_ref=stat_in.at[i],
            send_sem=s1_send.at[i], recv_sem=s1_recv.at[i],
            device_id=(base + partner(pos, i),), device_id_type=pl.DeviceIdType.MESH)

    def group_copy(k):
        return pltpu.make_async_remote_copy(
            src_ref=group_own, dst_ref=group_in.at[k],
            send_sem=s2_send.at[k], recv_sem=s2_recv.at[k],
            device_id=(far_partner(me, k),), device_id_type=pl.DeviceIdType.MESH)

    lane = lax.broadcasted_iota(jnp.int32, (8, LANES), 1)
    row = lax.broadcasted_iota(jnp.int32, (8, LANES), 0)
    block = lane // 32
    order = [((q + lane % 4) % 4) * 32 + lane // 4 for q in range(4)]

    def work(i, carry, store):
        load_px(i).wait()
        load_fl(i).wait()
        low, high, count, total, square = carry
        low, high, count, total, square = list(low), list(high), list(count), list(total), list(square)
        sums = [[] for _ in range(BANDS)]
        squares = [[] for _ in range(BANDS)]
        for r in range(2):
            for j in range(4):
                turned = []
                for b in range(BANDS):
                    value = px[i, b, pl.ds(8 * r, 8), pl.ds(LANES * j, LANES)]
                    flag = fl[i, b, pl.ds(8 * r, 8), pl.ds(LANES * j, LANES)]
                    usable = flag == 1
                    filled = jnp.where(usable, value, 0.0)
                    low[b] = jnp.minimum(low[b], jnp.where(usable, value, LARGEST))
                    high[b] = jnp.maximum(high[b], jnp.where(usable, value, -LARGEST))
                    count[b] = count[b] + flag
                    sums[b].append(filled)
                    squares[b].append(filled * filled)
                    turned.append(filled if b == 0 else pltpu.roll(filled, 32 * b, 1))
                for q in range(4):
                    mixed = turned[(0 - q) % 4]
                    for k in range(1, 4):
                        mixed = jnp.where(block == k, turned[(k - q) % 4], mixed)
                    store(r, j * 4 + q, jnp.take_along_axis(mixed, order[q], axis=1))

        def tree(parts):
            while len(parts) > 1:
                parts = [a + b for a, b in zip(parts[::2], parts[1::2])]
            return parts[0]

        for b in range(BANDS):
            total[b] = total[b] + tree(sums[b])
            square[b] = square[b] + tree(squares[b])
        return (tuple(low), tuple(high), tuple(count), tuple(total), tuple(square))

    zero = jnp.zeros((8, LANES), jnp.float32)
    carry = (
        (zero + LARGEST,) * BANDS, (zero - LARGEST,) * BANDS,
        (jnp.zeros((8, LANES), jnp.int32),) * BANDS, (zero,) * BANDS, (zero,) * BANDS,
    )

    def step(i, carry):
        def store(r, c, value):
            send[i, pl.ds(8 * r, 8), pl.ds(LANES * c, LANES)] = value

        carry = work(i, carry, store)

        @pl.when(i == 0)
        def _():
            pl.semaphore_wait(barrier, 22)

        @pl.when(i < EARLY)
        def _():
            piece(i).start()

        return carry

    carry = lax.fori_loop(0, 15, step, carry)

    def store_own(r, c, value):
        out[pl.ds(pl.multiple_of(my_rows + 8 * r, 8), 8), pl.ds(LANES * c, LANES)] = value

    low, high, count, total, square = work(15, carry, store_own)

    stats = jnp.zeros((8, LANES), jnp.float32)
    for b in range(BANDS):
        for s, value in enumerate((
            jnp.min(low[b], axis=(0, 1), keepdims=True),
            jnp.max(high[b], axis=(0, 1), keepdims=True),
            jnp.sum(count[b].astype(jnp.float32), axis=(0, 1), keepdims=True),
            jnp.sum(total[b], axis=(0, 1), keepdims=True),
            jnp.sum(square[b], axis=(0, 1), keepdims=True),
        )):
            stats = jnp.where((row == b) & (lane == s), value, stats)
    stat_own[...] = stats

    def start_stat(i, _):
        stat_copy(i).start()
        return 0

    lax.fori_loop(0, 15, start_stat, 0)

    def start_late(i, _):
        piece(i).start()
        return 0

    lax.fori_loop(EARLY, 15, start_late, 0)

    def take_stat(i, acc):
        stat_copy(i).wait_recv()
        return merge(acc, stat_in[i], lane)

    acc = lax.fori_loop(0, 15, take_stat, stat_own[...])
    group_own[...] = acc

    def start_group(k, _):
        group_copy(k).start()
        return 0

    lax.fori_loop(1, 8, start_group, 0)

    def take_group(k, acc):
        group_copy(k).wait_recv()
        return merge(acc, group_in[k], lane)

    acc = lax.fori_loop(1, 8, take_group, acc)
    low, high, valid = acc[:, 0:1], acc[:, 1:2], acc[:, 2:3]
    divisor = jnp.maximum(valid, 1.0)
    average = acc[:, 3:4] / divisor
    variance = acc[:, 4:5] / divisor - average * average
    deviation = jnp.sqrt(jnp.maximum(variance, 0.25))
    table = jnp.where(lane == 0, low, jnp.where(lane == 1, high, jnp.where(
        lane == 2, valid / CELLS, jnp.where(lane == 3, average, deviation))))
    header[...] = table[:BANDS, :5]

    def finish(i, _):
        piece(i).wait_send()
        piece(i).wait_recv()
        stat_copy(i).wait_send()
        return 0

    lax.fori_loop(0, 15, finish, 0)

    def finish_far(k, _):
        group_copy(k).wait_send()
        return 0

    lax.fori_loop(1, 8, finish_far, 0)


def on_device(pixels, valid_flags):
    dma = pltpu.SemaphoreType.DMA
    tile, header = pl.pallas_call(
        kernel,
        out_shape=(
            jax.ShapeDtypeStruct((HALF, WIDE), jnp.float32),
            jax.ShapeDtypeStruct((BANDS, 5), jnp.float32),
        ),
        in_specs=[pl.BlockSpec(memory_space=pltpu.HBM)] * 2,
        out_specs=(pl.BlockSpec(memory_space=pltpu.VMEM), pl.BlockSpec(memory_space=pltpu.VMEM)),
        scratch_shapes=[
            pltpu.VMEM((GROUP, BANDS, STRIP, TILE), jnp.float32),
            pltpu.VMEM((GROUP, BANDS, STRIP, TILE), jnp.int32),
            pltpu.VMEM((GROUP - 1, STRIP, WIDE), jnp.float32),
            pltpu.VMEM((8, LANES), jnp.float32),
            pltpu.VMEM((GROUP - 1, 8, LANES), jnp.float32),
            pltpu.VMEM((8, LANES), jnp.float32),
            pltpu.VMEM((8, 8, LANES), jnp.float32),
            dma((2, GROUP)), dma((GROUP - 1,)), dma((GROUP - 1,)),
            dma((GROUP - 1,)), dma((GROUP - 1,)), dma((8,)), dma((8,)),
        ],
        compiler_params=pltpu.CompilerParams(collective_id=0, has_side_effects=True, vmem_limit_bytes=16 * 1024 * 1024),
        name="export",
    )(pltpu.with_memory_space_constraint(pixels, pltpu.HBM), pltpu.with_memory_space_constraint(valid_flags, pltpu.HBM))
    return tile.reshape(1, HALF, WIDE), header.T


def solution(mesh):
    placed = (P(None, "dev", None), P(None, "dev", None))
    return jax.shard_map(
        on_device, mesh=mesh, in_specs=placed, out_specs=(P("dev", None, None), P()), check_vma=False
    )
```

```python
import jax
import jax.numpy as jnp
from jax import lax
from jax.experimental import pallas as pl
from jax.experimental.pallas import tpu as pltpu
from jax.sharding import PartitionSpec as P

BANDS = 4
TILE = 512
STRIP = 16
GROUP = 16
HALF = 256
N_DEV = 128
WIDE = TILE * BANDS
CELLS = 16777216.0
LARGEST = 3e38
LANES = 128
EARLY = 10


STEPS = (
    (1, 2, 0), (0, 2, 0), (1, 2, 1), (0, 2, 1), (1, 1, 0), (0, 3, 0), (1, 3, 0), (0, 1, 0),
    (1, 1, 1), (0, 3, 1), (1, 3, 1), (0, 1, 1), (1, 0, 0), (1, 0, 1), (0, 0, 1), (0, 0, 0),
)
CODES = [sum((z * 8 + y * 2 + c) << (4 * k) for k, (z, y, c) in enumerate(STEPS[at:at + 7])) for at in (0, 7, 14)]


def partner(pos, i):
    code = jnp.where(i < 7, CODES[0], jnp.where(i < 14, CODES[1], CODES[2]))
    code = (code >> (4 * (i % 7))) % 16
    dz, dy, dc = code // 8, (code // 2) % 4, code % 2
    z, y, c = pos // 8, (pos // 2) % 4, pos % 2
    return ((z + dz) % 2) * 8 + ((y + dy) % 4) * 2 + (c + dc) % 2


def far_partner(me, k):
    group, pos = me // GROUP, me % GROUP
    return ((group + k) % 8) * GROUP + pos


def merge(a, b, lane):
    return jnp.where(lane == 0, jnp.minimum(a, b), jnp.where(lane == 1, jnp.maximum(a, b), a + b))


def kernel(px_hbm, fl_hbm, out, header, px, fl, send, stat_own, stat_in, group_own, group_in,
           in_sem, send_sem, recv_sem, s1_send, s1_recv, s2_send, s2_recv):
    me = lax.axis_index("dev")
    base = (me // GROUP) * GROUP
    pos = me % GROUP
    group = me // GROUP

    def load_px(i):
        at = pl.multiple_of(partner(pos, i) * TILE, TILE)
        return pltpu.make_async_copy(px_hbm.at[:, :, pl.ds(at, TILE)], px.at[i], in_sem.at[0, i])

    def load_fl(i):
        at = pl.multiple_of(partner(pos, i) * TILE, TILE)
        return pltpu.make_async_copy(fl_hbm.at[:, :, pl.ds(at, TILE)], fl.at[i], in_sem.at[1, i])

    def start_load(i, _):
        load_px(i).start()
        load_fl(i).start()
        return 0

    lax.fori_loop(0, GROUP, start_load, 0)

    barrier = pltpu.get_barrier_semaphore()

    def greet(i, _):
        pl.semaphore_signal(barrier, inc=1, device_id=(base + partner(pos, i),),
                            device_id_type=pl.DeviceIdType.MESH)
        return 0

    def greet_far(k, _):
        @pl.when((group + k) % 8 > group)
        def _():
            pl.semaphore_signal(barrier, inc=1, device_id=(far_partner(me, k),),
                                device_id_type=pl.DeviceIdType.MESH)

        return 0

    lax.fori_loop(0, 15, greet, 0)
    lax.fori_loop(1, 8, greet_far, 0)

    my_rows = pl.multiple_of(pos * STRIP, STRIP)

    def piece(i):
        return pltpu.make_async_remote_copy(
            src_ref=send.at[i], dst_ref=out.at[pl.ds(my_rows, STRIP)],
            send_sem=send_sem.at[i], recv_sem=recv_sem.at[i],
            device_id=(base + partner(pos, i),), device_id_type=pl.DeviceIdType.MESH)

    def stat_copy(i):
        return pltpu.make_async_remote_copy(
            src_ref=stat_own, dst_ref=stat_in.at[i],
            send_sem=s1_send.at[i], recv_sem=s1_recv.at[i],
            device_id=(base + partner(pos, i),), device_id_type=pl.DeviceIdType.MESH)

    def group_copy(k):
        return pltpu.make_async_remote_copy(
            src_ref=group_own, dst_ref=group_in.at[k],
            send_sem=s2_send.at[k], recv_sem=s2_recv.at[k],
            device_id=(far_partner(me, k),), device_id_type=pl.DeviceIdType.MESH)

    lane = lax.broadcasted_iota(jnp.int32, (8, LANES), 1)
    row = lax.broadcasted_iota(jnp.int32, (8, LANES), 0)
    block = lane // 32
    order = [((q + lane % 4) % 4) * 32 + lane // 4 for q in range(4)]

    def work(i, carry, store):
        load_px(i).wait()
        load_fl(i).wait()
        low, high, count, total, square = carry
        low, high, count, total, square = list(low), list(high), list(count), list(total), list(square)
        sums = [[] for _ in range(BANDS)]
        squares = [[] for _ in range(BANDS)]
        for r in range(2):
            for j in range(4):
                turned = []
                for b in range(BANDS):
                    value = px[i, b, pl.ds(8 * r, 8), pl.ds(LANES * j, LANES)]
                    flag = fl[i, b, pl.ds(8 * r, 8), pl.ds(LANES * j, LANES)]
                    usable = flag == 1
                    filled = jnp.where(usable, value, 0.0)
                    low[b] = jnp.minimum(low[b], jnp.where(usable, value, LARGEST))
                    high[b] = jnp.maximum(high[b], jnp.where(usable, value, -LARGEST))
                    count[b] = count[b] + flag
                    sums[b].append(filled)
                    squares[b].append(filled * filled)
                    turned.append(filled if b == 0 else pltpu.roll(filled, 32 * b, 1))
                for q in range(4):
                    mixed = turned[(0 - q) % 4]
                    for k in range(1, 4):
                        mixed = jnp.where(block == k, turned[(k - q) % 4], mixed)
                    store(r, j * 4 + q, jnp.take_along_axis(mixed, order[q], axis=1))

        def tree(parts):
            while len(parts) > 1:
                parts = [a + b for a, b in zip(parts[::2], parts[1::2])]
            return parts[0]

        for b in range(BANDS):
            total[b] = total[b] + tree(sums[b])
            square[b] = square[b] + tree(squares[b])
        return (tuple(low), tuple(high), tuple(count), tuple(total), tuple(square))

    zero = jnp.zeros((8, LANES), jnp.float32)
    carry = (
        (zero + LARGEST,) * BANDS, (zero - LARGEST,) * BANDS,
        (jnp.zeros((8, LANES), jnp.int32),) * BANDS, (zero,) * BANDS, (zero,) * BANDS,
    )

    def step(i, carry):
        def store(r, c, value):
            send[i, pl.ds(8 * r, 8), pl.ds(LANES * c, LANES)] = value

        carry = work(i, carry, store)

        @pl.when(i == 0)
        def _():
            pl.semaphore_wait(barrier, 15 + group)

        @pl.when(i < EARLY)
        def _():
            piece(i).start()

        return carry

    carry = lax.fori_loop(0, 15, step, carry)

    def store_own(r, c, value):
        out[pl.ds(pl.multiple_of(my_rows + 8 * r, 8), 8), pl.ds(LANES * c, LANES)] = value

    low, high, count, total, square = work(15, carry, store_own)

    stats = jnp.zeros((8, LANES), jnp.float32)
    for b in range(BANDS):
        for s, value in enumerate((
            jnp.min(low[b], axis=(0, 1), keepdims=True),
            jnp.max(high[b], axis=(0, 1), keepdims=True),
            jnp.sum(count[b].astype(jnp.float32), axis=(0, 1), keepdims=True),
            jnp.sum(total[b], axis=(0, 1), keepdims=True),
            jnp.sum(square[b], axis=(0, 1), keepdims=True),
        )):
            stats = jnp.where((row == b) & (lane == s), value, stats)
    stat_own[...] = stats

    def start_stat(i, _):
        stat_copy(i).start()
        return 0

    lax.fori_loop(0, 15, start_stat, 0)

    def start_late(i, _):
        piece(i).start()
        return 0

    lax.fori_loop(EARLY, 15, start_late, 0)

    def take_stat(i, acc):
        stat_copy(i).wait_recv()
        return merge(acc, stat_in[i], lane)

    acc = lax.fori_loop(0, 15, take_stat, stat_own[...])
    group_own[...] = acc

    def to_lower(k, _):
        @pl.when((group + k) % 8 < group)
        def _():
            group_copy(k).start()

        return 0

    lax.fori_loop(1, 8, to_lower, 0)

    def to_higher(k, _):
        @pl.when((group + 8 - k) % 8 > group)
        def _():
            group_copy(k).wait_recv()
            group_copy(8 - k).start()

        return 0

    lax.fori_loop(1, 8, to_higher, 0)

    def from_lower(k, _):
        @pl.when((group + 8 - k) % 8 < group)
        def _():
            group_copy(k).wait_recv()

        return 0

    lax.fori_loop(1, 8, from_lower, 0)

    def take_group(k, acc):
        return merge(acc, group_in[k], lane)

    acc = lax.fori_loop(1, 8, take_group, acc)
    low, high, valid = acc[:, 0:1], acc[:, 1:2], acc[:, 2:3]
    divisor = jnp.maximum(valid, 1.0)
    average = acc[:, 3:4] / divisor
    variance = acc[:, 4:5] / divisor - average * average
    deviation = jnp.sqrt(jnp.maximum(variance, 0.25))
    table = jnp.where(lane == 0, low, jnp.where(lane == 1, high, jnp.where(
        lane == 2, valid / CELLS, jnp.where(lane == 3, average, deviation))))
    header[...] = table[:BANDS, :5]

    def finish(i, _):
        piece(i).wait_send()
        piece(i).wait_recv()
        stat_copy(i).wait_send()
        return 0

    lax.fori_loop(0, 15, finish, 0)

    def finish_far(k, _):
        group_copy(k).wait_send()
        return 0

    lax.fori_loop(1, 8, finish_far, 0)


def on_device(pixels, valid_flags):
    dma = pltpu.SemaphoreType.DMA
    tile, header = pl.pallas_call(
        kernel,
        out_shape=(
            jax.ShapeDtypeStruct((HALF, WIDE), jnp.float32),
            jax.ShapeDtypeStruct((BANDS, 5), jnp.float32),
        ),
        in_specs=[pl.BlockSpec(memory_space=pltpu.HBM)] * 2,
        out_specs=(pl.BlockSpec(memory_space=pltpu.VMEM), pl.BlockSpec(memory_space=pltpu.VMEM)),
        scratch_shapes=[
            pltpu.VMEM((GROUP, BANDS, STRIP, TILE), jnp.float32),
            pltpu.VMEM((GROUP, BANDS, STRIP, TILE), jnp.int32),
            pltpu.VMEM((GROUP - 1, STRIP, WIDE), jnp.float32),
            pltpu.VMEM((8, LANES), jnp.float32),
            pltpu.VMEM((GROUP - 1, 8, LANES), jnp.float32),
            pltpu.VMEM((8, LANES), jnp.float32),
            pltpu.VMEM((8, 8, LANES), jnp.float32),
            dma((2, GROUP)), dma((GROUP - 1,)), dma((GROUP - 1,)),
            dma((GROUP - 1,)), dma((GROUP - 1,)), dma((8,)), dma((8,)),
        ],
        compiler_params=pltpu.CompilerParams(collective_id=0, has_side_effects=True, vmem_limit_bytes=16 * 1024 * 1024),
        name="export",
    )(pltpu.with_memory_space_constraint(pixels, pltpu.HBM), pltpu.with_memory_space_constraint(valid_flags, pltpu.HBM))
    return tile.reshape(1, HALF, WIDE), header.T


def solution(mesh):
    placed = (P(None, "dev", None), P(None, "dev", None))
    return jax.shard_map(
        on_device, mesh=mesh, in_specs=placed, out_specs=(P("dev", None, None), P()), check_vma=False
    )
```

```python
import jax
import jax.numpy as jnp
from jax import lax
from jax.experimental import pallas as pl
from jax.experimental.pallas import tpu as pltpu
from jax.sharding import PartitionSpec as P

BANDS = 4
TILE = 512
STRIP = 16
GROUP = 16
HALF = 256
WIDE = TILE * BANDS
CELLS = 16777216.0
LARGEST = 3e38
LANES = 128
EARLY = 5
MESH = pl.DeviceIdType.MESH

STEPS = (
    (1, 2, 0), (0, 2, 0), (1, 2, 1), (0, 2, 1), (1, 1, 0), (0, 3, 0), (1, 3, 0), (0, 1, 0),
    (1, 1, 1), (0, 3, 1), (1, 3, 1), (0, 1, 1), (1, 0, 0), (1, 0, 1), (0, 0, 1), (0, 0, 0),
)
NIBBLES = [z * 8 + y * 2 + c for z, y, c in STEPS]


def packed(part):
    value = sum(code << (4 * k) for k, code in enumerate(part))
    return value - (1 << 32) if value >= 1 << 31 else value


FIRST, SECOND = packed(NIBBLES[:8]), packed(NIBBLES[8:])


def partner(pos, i):
    if isinstance(i, int):
        code = NIBBLES[i]
    else:
        code = (jnp.where(i < 8, FIRST, SECOND) >> ((i & 7) * 4)) & 15
    return ((pos ^ code) & 9) | ((pos + (code & 6)) & 6)


def far_partner(group, pos, k):
    other = ((group + 2 * (k % 4)) & 7) ^ (k // 4)
    return other, pos ^ (8 * (k // 4))


def merge(a, b, lane):
    return jnp.where(lane == 0, jnp.minimum(a, b), jnp.where(lane == 1, jnp.maximum(a, b), a + b))


def kernel(px_hbm, fl_hbm, out, header, px, fl, send, stat, total, in_sem, send_sem, recv_sem,
           s1_send, s1_recv, s2_send, s2_recv):
    me = lax.axis_index("dev")
    pos = me & 15
    group = me >> 4
    base = me - pos

    def load_px(i):
        at = pl.multiple_of(partner(pos, i) * TILE, TILE)
        return pltpu.make_async_copy(px_hbm.at[:, :, pl.ds(at, TILE)], px.at[i], in_sem.at[0, i])

    def load_fl(i):
        at = pl.multiple_of(partner(pos, i) * TILE, TILE)
        return pltpu.make_async_copy(fl_hbm.at[:, :, pl.ds(at, TILE)], fl.at[i], in_sem.at[1, i])

    for i in range(GROUP):
        load_px(i).start()
        load_fl(i).start()

    barrier = pltpu.get_barrier_semaphore()
    for i in range(15):
        pl.semaphore_signal(barrier, inc=1, device_id=(base + partner(pos, i),), device_id_type=MESH)
    for k in range(1, 8):
        other, there = far_partner(group, pos, k)

        @pl.when(other > group)
        def _():
            pl.semaphore_signal(barrier, inc=1, device_id=(other * GROUP + there,), device_id_type=MESH)

    my_rows = pl.multiple_of(pos * STRIP, STRIP)

    def piece(i):
        return pltpu.make_async_remote_copy(
            src_ref=send.at[i], dst_ref=out.at[pl.ds(my_rows, STRIP)],
            send_sem=send_sem.at[i], recv_sem=recv_sem.at[i],
            device_id=(base + partner(pos, i),), device_id_type=MESH)

    def stat_copy(i):
        return pltpu.make_async_remote_copy(
            src_ref=stat.at[pos], dst_ref=stat.at[pos],
            send_sem=s1_send.at[i], recv_sem=s1_recv.at[i],
            device_id=(base + partner(pos, i),), device_id_type=MESH)

    def total_copy(k):
        other, there = far_partner(group, pos, k)
        return pltpu.make_async_remote_copy(
            src_ref=total.at[group], dst_ref=total.at[group],
            send_sem=s2_send.at[k], recv_sem=s2_recv.at[k],
            device_id=(other * GROUP + there,), device_id_type=MESH)

    lane = lax.broadcasted_iota(jnp.int32, (8, LANES), 1)
    row = lax.broadcasted_iota(jnp.int32, (8, LANES), 0)
    block = lane // 32
    order = [((q + lane % 4) % 4) * 32 + lane // 4 for q in range(4)]

    def work(i, carry, store):
        load_px(i).wait()
        load_fl(i).wait()
        low, high, count, summed, square = [list(part) for part in carry]
        sums = [[] for _ in range(BANDS)]
        squares = [[] for _ in range(BANDS)]
        for r in range(2):
            for j in range(4):
                turned = []
                for b in range(BANDS):
                    value = px[i, b, pl.ds(8 * r, 8), pl.ds(LANES * j, LANES)]
                    flag = fl[i, b, pl.ds(8 * r, 8), pl.ds(LANES * j, LANES)]
                    usable = flag == 1
                    filled = jnp.where(usable, value, 0.0)
                    low[b] = jnp.minimum(low[b], jnp.where(usable, value, LARGEST))
                    high[b] = jnp.maximum(high[b], jnp.where(usable, value, -LARGEST))
                    count[b] = count[b] + flag
                    sums[b].append(filled)
                    squares[b].append(filled * filled)
                    turned.append(filled if b == 0 else pltpu.roll(filled, 32 * b, 1))
                for q in range(4):
                    mixed = turned[(0 - q) % 4]
                    for k in range(1, 4):
                        mixed = jnp.where(block == k, turned[(k - q) % 4], mixed)
                    store(r, j * 4 + q, jnp.take_along_axis(mixed, order[q], axis=1))

        def tree(parts):
            while len(parts) > 1:
                parts = [a + b for a, b in zip(parts[::2], parts[1::2])]
            return parts[0]

        for b in range(BANDS):
            summed[b] = summed[b] + tree(sums[b])
            square[b] = square[b] + tree(squares[b])
        return tuple(tuple(part) for part in (low, high, count, summed, square))

    zero = jnp.zeros((8, LANES), jnp.float32)
    carry = (
        (zero + LARGEST,) * BANDS, (zero - LARGEST,) * BANDS,
        (jnp.zeros((8, LANES), jnp.int32),) * BANDS, (zero,) * BANDS, (zero,) * BANDS,
    )

    def step(i, carry):
        def store(r, c, value):
            send[i, pl.ds(8 * r, 8), pl.ds(LANES * c, LANES)] = value

        carry = work(i, carry, store)

        @pl.when(i == 0)
        def _():
            pl.semaphore_wait(barrier, 15 + group)

        @pl.when(i < EARLY)
        def _():
            piece(i).start()

        return carry

    carry = lax.fori_loop(0, 15, step, carry)

    def store_own(r, c, value):
        out[pl.ds(pl.multiple_of(my_rows + 8 * r, 8), 8), pl.ds(LANES * c, LANES)] = value

    low, high, count, summed, square = work(15, carry, store_own)

    stats = zero
    for b in range(BANDS):
        for s, value in enumerate((
            jnp.min(low[b], axis=(0, 1), keepdims=True),
            jnp.max(high[b], axis=(0, 1), keepdims=True),
            jnp.sum(count[b].astype(jnp.float32), axis=(0, 1), keepdims=True),
            jnp.sum(summed[b], axis=(0, 1), keepdims=True),
            jnp.sum(square[b], axis=(0, 1), keepdims=True),
        )):
            stats = jnp.where((row == b) & (lane == s), value, stats)
    stat[pos] = stats

    for i in range(15):
        stat_copy(i).start()
    for i in range(EARLY, 15):
        piece(i).start()

    for i in range(15):
        stat_copy(i).wait_recv()
    acc = stat[0]
    for k in range(1, GROUP):
        acc = merge(acc, stat[k], lane)
    total[group] = acc

    for k in range(1, 8):
        @pl.when(far_partner(group, pos, k)[0] < group)
        def _():
            total_copy(k).start()

    back = [None, 3, 2, 1, 4, 7, 6, 5]
    for k in range(1, 8):
        @pl.when(far_partner(group, pos, back[k])[0] > group)
        def _():
            total_copy(k).wait_recv()
            total_copy(back[k]).start()

    for k in range(1, 8):
        @pl.when(far_partner(group, pos, back[k])[0] < group)
        def _():
            total_copy(k).wait_recv()

    acc = total[0]
    for k in range(1, 8):
        acc = merge(acc, total[k], lane)
    low, high, valid = acc[:, 0:1], acc[:, 1:2], acc[:, 2:3]
    divisor = jnp.maximum(valid, 1.0)
    average = acc[:, 3:4] / divisor
    variance = acc[:, 4:5] / divisor - average * average
    deviation = jnp.sqrt(jnp.maximum(variance, 0.25))
    table = jnp.where(lane == 0, low, jnp.where(lane == 1, high, jnp.where(
        lane == 2, valid / CELLS, jnp.where(lane == 3, average, deviation))))
    header[...] = table[:BANDS, :5]

    for k in range(1, 8):
        total_copy(k).wait_send()
    for i in range(15):
        stat_copy(i).wait_send()
        piece(i).wait_send()
        piece(i).wait_recv()


def on_device(pixels, valid_flags):
    dma = pltpu.SemaphoreType.DMA
    tile, header = pl.pallas_call(
        kernel,
        out_shape=(
            jax.ShapeDtypeStruct((HALF, WIDE), jnp.float32),
            jax.ShapeDtypeStruct((BANDS, 5), jnp.float32),
        ),
        in_specs=[pl.BlockSpec(memory_space=pltpu.HBM)] * 2,
        out_specs=(pl.BlockSpec(memory_space=pltpu.VMEM), pl.BlockSpec(memory_space=pltpu.VMEM)),
        scratch_shapes=[
            pltpu.VMEM((GROUP, BANDS, STRIP, TILE), jnp.float32),
            pltpu.VMEM((GROUP, BANDS, STRIP, TILE), jnp.int32),
            pltpu.VMEM((GROUP - 1, STRIP, WIDE), jnp.float32),
            pltpu.VMEM((GROUP, 8, LANES), jnp.float32),
            pltpu.VMEM((8, 8, LANES), jnp.float32),
            dma((2, GROUP)), dma((GROUP - 1,)), dma((GROUP - 1,)),
            dma((GROUP - 1,)), dma((GROUP - 1,)), dma((8,)), dma((8,)),
        ],
        compiler_params=pltpu.CompilerParams(
            collective_id=0, has_side_effects=True, vmem_limit_bytes=16 * 1024 * 1024),
        name="export",
    )(
        pltpu.with_memory_space_constraint(pixels, pltpu.HBM),
        pltpu.with_memory_space_constraint(valid_flags, pltpu.HBM),
    )
    return tile.reshape(1, HALF, WIDE), header.T


def solution(mesh):
    placed = (P(None, "dev", None), P(None, "dev", None))
    return jax.shard_map(
        on_device, mesh=mesh, in_specs=placed, out_specs=(P("dev", None, None), P()), check_vma=False
    )
```

```python
import jax
import jax.numpy as jnp
from jax import lax
from jax.experimental import pallas as pl
from jax.experimental.pallas import tpu as pltpu
from jax.sharding import PartitionSpec as P

BANDS = 4
TILE = 512
STRIP = 16
GROUP = 16
HALF = 256
WIDE = TILE * BANDS
CELLS = 16777216.0
LARGEST = 3e38
LANES = 128
EARLY = 5
PARTS = 4
MESH = pl.DeviceIdType.MESH

STEPS = (
    (1, 2, 0), (0, 2, 0), (1, 2, 1), (0, 2, 1), (1, 1, 0), (0, 3, 0), (1, 3, 0), (0, 1, 0),
    (1, 1, 1), (0, 3, 1), (1, 3, 1), (0, 1, 1), (1, 0, 0), (1, 0, 1), (0, 0, 1), (0, 0, 0),
)
NIBBLES = [z * 8 + y * 2 + c for z, y, c in STEPS]


def packed(part):
    value = sum(code << (4 * k) for k, code in enumerate(part))
    return value - (1 << 32) if value >= 1 << 31 else value


FIRST, SECOND = packed(NIBBLES[:8]), packed(NIBBLES[8:])


def partner(pos, i):
    if isinstance(i, int):
        code = NIBBLES[i]
    else:
        code = (jnp.where(i < 8, FIRST, SECOND) >> ((i & 7) * 4)) & 15
    return ((pos ^ code) & 9) | ((pos + (code & 6)) & 6)


def far_partner(group, pos, k):
    other = ((group + 2 * (k % 4)) & 7) ^ (k // 4)
    return other, pos ^ (8 * (k // 4))


def merge(a, b, lane):
    return jnp.where(lane == 0, jnp.minimum(a, b), jnp.where(lane == 1, jnp.maximum(a, b), a + b))


def kernel(px_hbm, fl_hbm, out, header, px, fl, send, stat, total, in_sem, send_sem, recv_sem,
           s1_send, s1_recv, s2_send, s2_recv, ready):
    me = lax.axis_index("dev")
    pos = me & 15
    group = me >> 4
    base = me - pos

    def load_px(i):
        at = pl.multiple_of(partner(pos, i) * TILE, TILE)
        return pltpu.make_async_copy(px_hbm.at[:, :, pl.ds(at, TILE)], px.at[i], in_sem.at[0, i])

    def load_fl(i):
        at = pl.multiple_of(partner(pos, i) * TILE, TILE)
        return pltpu.make_async_copy(fl_hbm.at[:, :, pl.ds(at, TILE)], fl.at[i], in_sem.at[1, i])

    for i in range(GROUP):
        load_px(i).start()
        load_fl(i).start()

    barrier = pltpu.get_barrier_semaphore()
    for i in range(15):
        pl.semaphore_signal(barrier, inc=1, device_id=(base + partner(pos, i),), device_id_type=MESH)
    for k in range(1, 8):
        other, there = far_partner(group, pos, k)

        @pl.when(other > group)
        def _():
            pl.semaphore_signal(barrier, inc=1, device_id=(other * GROUP + there,), device_id_type=MESH)

    my_rows = pl.multiple_of(pos * STRIP, STRIP)

    def piece(i):
        return pltpu.make_async_remote_copy(
            src_ref=send.at[i], dst_ref=out.at[pl.ds(my_rows, STRIP)],
            send_sem=send_sem.at[i], recv_sem=recv_sem.at[i],
            device_id=(base + partner(pos, i),), device_id_type=MESH)

    def stat_copy(i):
        return pltpu.make_async_remote_copy(
            src_ref=stat.at[pos], dst_ref=stat.at[pos],
            send_sem=s1_send.at[i], recv_sem=s1_recv.at[i],
            device_id=(base + partner(pos, i),), device_id_type=MESH)

    def total_copy(k):
        other, there = far_partner(group, pos, k)
        return pltpu.make_async_remote_copy(
            src_ref=total.at[group], dst_ref=total.at[group],
            send_sem=s2_send.at[k], recv_sem=s2_recv.at[k],
            device_id=(other * GROUP + there,), device_id_type=MESH)

    lane = lax.broadcasted_iota(jnp.int32, (8, LANES), 1)
    row = lax.broadcasted_iota(jnp.int32, (8, LANES), 0)
    block = lane // 32
    order = [((q + lane % 4) % 4) * 32 + lane // 4 for q in range(4)]

    def work(i, carry, store):
        load_px(i).wait()
        load_fl(i).wait()
        low, high, count, summed, square = [list(part) for part in carry]
        sums = [[] for _ in range(BANDS)]
        squares = [[] for _ in range(BANDS)]
        for r in range(2):
            for j in range(4):
                turned = []
                for b in range(BANDS):
                    value = px[i, b, pl.ds(8 * r, 8), pl.ds(LANES * j, LANES)]
                    flag = fl[i, b, pl.ds(8 * r, 8), pl.ds(LANES * j, LANES)]
                    usable = flag == 1
                    filled = jnp.where(usable, value, 0.0)
                    low[b] = jnp.minimum(low[b], jnp.where(usable, value, LARGEST))
                    high[b] = jnp.maximum(high[b], jnp.where(usable, value, -LARGEST))
                    count[b] = count[b] + flag
                    sums[b].append(filled)
                    squares[b].append(filled * filled)
                    turned.append(filled if b == 0 else pltpu.roll(filled, 32 * b, 1))
                for q in range(4):
                    mixed = turned[(0 - q) % 4]
                    for k in range(1, 4):
                        mixed = jnp.where(block == k, turned[(k - q) % 4], mixed)
                    store(r, j * 4 + q, jnp.take_along_axis(mixed, order[q], axis=1))

        def tree(parts):
            while len(parts) > 1:
                parts = [a + b for a, b in zip(parts[::2], parts[1::2])]
            return parts[0]

        for b in range(BANDS):
            summed[b] = summed[b] + tree(sums[b])
            square[b] = square[b] + tree(squares[b])
        return tuple(tuple(part) for part in (low, high, count, summed, square))

    zero = jnp.zeros((8, LANES), jnp.float32)
    carry = (
        (zero + LARGEST,) * BANDS, (zero - LARGEST,) * BANDS,
        (jnp.zeros((8, LANES), jnp.int32),) * BANDS, (zero,) * BANDS, (zero,) * BANDS,
    )

    def step(i, carry):
        def store(r, c, value):
            send[i, pl.ds(8 * r, 8), pl.ds(LANES * c, LANES)] = value

        carry = work(i, carry, store)

        @pl.when(i == 0)
        def _():
            pl.semaphore_wait(barrier, 15 + group)
            for k in range(1, 8):
                other, there = far_partner(group, pos, k)

                @pl.when(other < group)
                def _():
                    pl.semaphore_signal(ready, inc=1, device_id=(other * GROUP + there,), device_id_type=MESH)

        @pl.when(i < EARLY)
        def _():
            piece(i).start()

        return carry

    carry = lax.fori_loop(0, 15, step, carry)

    def store_own(r, c, value):
        out[pl.ds(pl.multiple_of(my_rows + 8 * r, 8), 8), pl.ds(LANES * c, LANES)] = value

    low, high, count, summed, square = work(15, carry, store_own)

    stats = zero
    for b in range(BANDS):
        for s, value in enumerate((
            jnp.min(low[b], axis=(0, 1), keepdims=True),
            jnp.max(high[b], axis=(0, 1), keepdims=True),
            jnp.sum(count[b].astype(jnp.float32), axis=(0, 1), keepdims=True),
            jnp.sum(summed[b], axis=(0, 1), keepdims=True),
            jnp.sum(square[b], axis=(0, 1), keepdims=True),
        )):
            stats = jnp.where((row == b) & (lane == s), value, stats)
    stat[pos] = stats

    for i in range(15):
        stat_copy(i).start()
    for i in range(EARLY, 15):
        piece(i).start()

    for i in range(15):
        stat_copy(i).wait_recv()
    acc = stat[0]
    for k in range(1, GROUP):
        acc = merge(acc, stat[k], lane)
    total[group] = acc
    @pl.when(group < 7)
    def _():
        pl.semaphore_wait(ready, 7 - group)

    for k in range(1, 8):
        total_copy(k).start()
    for k in range(1, 8):
        total_copy(k).wait_recv()

    acc = total[0]
    for k in range(1, 8):
        acc = merge(acc, total[k], lane)
    low, high, valid = acc[:, 0:1], acc[:, 1:2], acc[:, 2:3]
    divisor = jnp.maximum(valid, 1.0)
    average = acc[:, 3:4] / divisor
    variance = acc[:, 4:5] / divisor - average * average
    deviation = jnp.sqrt(jnp.maximum(variance, 0.25))
    table = jnp.where(lane == 0, low, jnp.where(lane == 1, high, jnp.where(
        lane == 2, valid / CELLS, jnp.where(lane == 3, average, deviation))))
    header[...] = table[:BANDS, :5]

    for k in range(1, 8):
        total_copy(k).wait_send()
    for i in range(15):
        stat_copy(i).wait_send()
        piece(i).wait_send()
        piece(i).wait_recv()


def place(tile, header, tile_out, header_out, sems):
    rows = HALF // PARTS
    copies = [pltpu.make_async_copy(header, header_out, sems.at[PARTS])] + [
        pltpu.make_async_copy(tile.at[pl.ds(rows * n, rows)], tile_out.at[pl.ds(rows * n, rows)], sems.at[n])
        for n in range(PARTS)
    ]
    for copy in copies:
        copy.start()
    for copy in copies:
        copy.wait()


def on_device(pixels, valid_flags):
    dma = pltpu.SemaphoreType.DMA
    tile, header = pl.pallas_call(
        kernel,
        out_shape=(
            jax.ShapeDtypeStruct((HALF, WIDE), jnp.float32),
            jax.ShapeDtypeStruct((BANDS, 5), jnp.float32),
        ),
        in_specs=[pl.BlockSpec(memory_space=pltpu.HBM)] * 2,
        out_specs=(pl.BlockSpec(memory_space=pltpu.VMEM), pl.BlockSpec(memory_space=pltpu.VMEM)),
        scratch_shapes=[
            pltpu.VMEM((GROUP, BANDS, STRIP, TILE), jnp.float32),
            pltpu.VMEM((GROUP, BANDS, STRIP, TILE), jnp.int32),
            pltpu.VMEM((GROUP - 1, STRIP, WIDE), jnp.float32),
            pltpu.VMEM((GROUP, 8, LANES), jnp.float32),
            pltpu.VMEM((8, 8, LANES), jnp.float32),
            dma((2, GROUP)), dma((GROUP - 1,)), dma((GROUP - 1,)),
            dma((GROUP - 1,)), dma((GROUP - 1,)), dma((8,)), dma((8,)),
            pltpu.SemaphoreType.REGULAR,
        ],
        compiler_params=pltpu.CompilerParams(
            collective_id=0, has_side_effects=True, vmem_limit_bytes=16 * 1024 * 1024),
        name="export",
    )(
        pltpu.with_memory_space_constraint(pixels, pltpu.HBM),
        pltpu.with_memory_space_constraint(valid_flags, pltpu.HBM),
    )
    tile, header = pl.pallas_call(
        place,
        out_shape=(
            jax.ShapeDtypeStruct((HALF, WIDE), jnp.float32),
            jax.ShapeDtypeStruct((BANDS, 5), jnp.float32),
        ),
        in_specs=[pl.BlockSpec(memory_space=pltpu.VMEM)] * 2,
        out_specs=(pl.BlockSpec(memory_space=pltpu.HBM), pl.BlockSpec(memory_space=pltpu.HBM)),
        scratch_shapes=[dma((PARTS + 1,))],
        compiler_params=pltpu.CompilerParams(vmem_limit_bytes=16 * 1024 * 1024),
        name="place",
    )(tile, header)
    return tile.reshape(1, HALF, WIDE), header.T


def solution(mesh):
    placed = (P(None, "dev", None), P(None, "dev", None))
    return jax.shard_map(
        on_device, mesh=mesh, in_specs=placed, out_specs=(P("dev", None, None), P()), check_vma=False
    )
```

```python
import jax
import jax.numpy as jnp
from jax import lax
from jax.experimental import pallas as pl
from jax.experimental.pallas import tpu as pltpu
from jax.sharding import PartitionSpec as P

BANDS = 4
TILE = 512
STRIP = 16
GROUP = 16
HALF = 256
WIDE = TILE * BANDS
CELLS = 16777216.0
LARGEST = 3e38
LANES = 128
EARLY = 2
LOADS = 2
PARTS = 4
MESH = pl.DeviceIdType.MESH

STEPS = (
    (1, 2, 0), (0, 2, 0), (1, 2, 1), (0, 2, 1), (1, 1, 0), (0, 3, 0), (1, 3, 0), (0, 1, 0),
    (1, 1, 1), (0, 3, 1), (1, 3, 1), (0, 1, 1), (1, 0, 0), (1, 0, 1), (0, 0, 1), (0, 0, 0),
)
NIBBLES = [z * 8 + y * 2 + c for z, y, c in STEPS]


def packed(part):
    value = sum(code << (4 * k) for k, code in enumerate(part))
    return value - (1 << 32) if value >= 1 << 31 else value


FIRST, SECOND = packed(NIBBLES[:8]), packed(NIBBLES[8:])


def moved(pos, code):
    return ((pos ^ code) & 9) | ((pos + (code & 6)) & 6)


def merge(a, b, lane):
    return jnp.where(lane == 0, jnp.minimum(a, b), jnp.where(lane == 1, jnp.maximum(a, b), a + b))


def kernel(px_hbm, fl_hbm, out, header, px, fl, send, stat, part, half, in_sem, send_sem, recv_sem,
           s1_send, s1_recv, s2_send, s2_recv, s3_send, s3_recv, ready_far):
    me = lax.axis_index("dev")
    pos = me & 15
    base = me - pos
    x = me >> 5
    high_z = (me >> 4) & 1
    first, second = FIRST, SECOND

    def target(i):
        return moved(pos, (jnp.where(i < 8, first, second) >> ((i & 7) * 4)) & 15)

    def x_partner(k):
        return (me + 32 * k) & 127

    across = me ^ 24

    def load_px(i):
        at = pl.multiple_of(target(i) * TILE, TILE)
        return pltpu.make_async_copy(px_hbm.at[:, :, pl.ds(at, TILE)], px.at[i], in_sem.at[0, i])

    def load_fl(i):
        at = pl.multiple_of(target(i) * TILE, TILE)
        return pltpu.make_async_copy(fl_hbm.at[:, :, pl.ds(at, TILE)], fl.at[i], in_sem.at[1, i])

    barrier = pltpu.get_barrier_semaphore()
    for i in range(LOADS):
        load_px(i).start()
        load_fl(i).start()
    for code in range(1, GROUP):
        pl.semaphore_signal(barrier, inc=1, device_id=(base + moved(pos, code),), device_id_type=MESH)
    for k in range(1, 4):
        @pl.when(x + k < 4)
        def _():
            pl.semaphore_signal(barrier, inc=1, device_id=(x_partner(k),), device_id_type=MESH)

    @pl.when(high_z == 0)
    def _():
        pl.semaphore_signal(barrier, inc=1, device_id=(across,), device_id_type=MESH)

    for i in range(LOADS, GROUP):
        load_px(i).start()
        load_fl(i).start()

    def enter():
        pl.semaphore_wait(barrier, 15 + x + high_z)
        for k in range(1, 4):
            @pl.when(x + k >= 4)
            def _():
                pl.semaphore_signal(ready_far.at[0], inc=1, device_id=(x_partner(k),), device_id_type=MESH)

        @pl.when(high_z == 1)
        def _():
            pl.semaphore_signal(ready_far.at[1], inc=1, device_id=(across,), device_id_type=MESH)

    my_rows = pl.multiple_of(pos * STRIP, STRIP)

    def piece(i):
        return pltpu.make_async_remote_copy(
            src_ref=send.at[i], dst_ref=out.at[pl.ds(my_rows, STRIP)],
            send_sem=send_sem.at[i], recv_sem=recv_sem.at[pos],
            device_id=(base + target(i),), device_id_type=MESH)

    def arrived(source):
        return pltpu.make_async_remote_copy(
            src_ref=send.at[0], dst_ref=out.at[pl.ds(my_rows, STRIP)],
            send_sem=send_sem.at[0], recv_sem=recv_sem.at[source],
            device_id=(base + source,), device_id_type=MESH)

    def stat_copy(code, slot):
        return pltpu.make_async_remote_copy(
            src_ref=stat.at[pos], dst_ref=stat.at[pos],
            send_sem=s1_send.at[code], recv_sem=s1_recv.at[slot],
            device_id=(base + moved(pos, code),), device_id_type=MESH)

    def part_copy(k):
        return pltpu.make_async_remote_copy(
            src_ref=part.at[x], dst_ref=part.at[x],
            send_sem=s2_send.at[k], recv_sem=s2_recv.at[k],
            device_id=(x_partner(k),), device_id_type=MESH)

    half_copy = pltpu.make_async_remote_copy(
        src_ref=half.at[high_z], dst_ref=half.at[high_z], send_sem=s3_send, recv_sem=s3_recv,
        device_id=(across,), device_id_type=MESH)

    lane = lax.broadcasted_iota(jnp.int32, (8, LANES), 1)
    row = lax.broadcasted_iota(jnp.int32, (8, LANES), 0)
    block = lane // 32
    order = [((q + lane % 4) % 4) * 32 + lane // 4 for q in range(4)]

    def work(i, carry, store):
        load_px(i).wait()
        load_fl(i).wait()
        low, high, count, summed, square = [list(part) for part in carry]
        sums = [[] for _ in range(BANDS)]
        squares = [[] for _ in range(BANDS)]
        for r in range(2):
            for j in range(4):
                turned = []
                for b in range(BANDS):
                    value = px[i, b, pl.ds(8 * r, 8), pl.ds(LANES * j, LANES)]
                    flag = fl[i, b, pl.ds(8 * r, 8), pl.ds(LANES * j, LANES)]
                    usable = flag == 1
                    filled = jnp.where(usable, value, 0.0)
                    low[b] = jnp.minimum(low[b], jnp.where(usable, value, LARGEST))
                    high[b] = jnp.maximum(high[b], jnp.where(usable, value, -LARGEST))
                    count[b] = count[b] + flag
                    sums[b].append(filled)
                    squares[b].append(filled * filled)
                    turned.append(filled if b == 0 else pltpu.roll(filled, 32 * b, 1))
                for q in range(4):
                    mixed = turned[(0 - q) % 4]
                    for k in range(1, 4):
                        mixed = jnp.where(block == k, turned[(k - q) % 4], mixed)
                    store(r, j * 4 + q, jnp.take_along_axis(mixed, order[q], axis=1))

        def tree(parts):
            while len(parts) > 1:
                parts = [a + b for a, b in zip(parts[::2], parts[1::2])]
            return parts[0]

        for b in range(BANDS):
            summed[b] = summed[b] + tree(sums[b])
            square[b] = square[b] + tree(squares[b])
        return tuple(tuple(part) for part in (low, high, count, summed, square))

    zero = jnp.zeros((8, LANES), jnp.float32)
    carry = (
        (zero + LARGEST,) * BANDS, (zero - LARGEST,) * BANDS,
        (jnp.zeros((8, LANES), jnp.int32),) * BANDS, (zero,) * BANDS, (zero,) * BANDS,
    )

    def step(i, carry):
        def store(r, c, value):
            send[i, pl.ds(8 * r, 8), pl.ds(LANES * c, LANES)] = value

        carry = work(i, carry, store)

        @pl.when(i == 0)
        def _():
            enter()

        @pl.when(i < EARLY)
        def _():
            piece(i).start()

        return carry

    carry = lax.fori_loop(0, 15, step, carry)

    def store_own(r, c, value):
        out[pl.ds(pl.multiple_of(my_rows + 8 * r, 8), 8), pl.ds(LANES * c, LANES)] = value

    low, high, count, summed, square = work(15, carry, store_own)

    stats = zero
    for b in range(BANDS):
        for s, value in enumerate((
            jnp.min(low[b], axis=(0, 1), keepdims=True),
            jnp.max(high[b], axis=(0, 1), keepdims=True),
            jnp.sum(count[b].astype(jnp.float32), axis=(0, 1), keepdims=True),
            jnp.sum(summed[b], axis=(0, 1), keepdims=True),
            jnp.sum(square[b], axis=(0, 1), keepdims=True),
        )):
            stats = jnp.where((row == b) & (lane == s), value, stats)
    stat[pos] = stats

    for code in reversed(range(1, GROUP)):
        stat_copy(code, pos).start()
    for i in range(EARLY, 15):
        piece(i).start()

    for code in range(1, GROUP):
        stat_copy(code, moved(pos, code)).wait_recv()
    acc = stat[0]
    for k in range(1, GROUP):
        acc = merge(acc, stat[k], lane)
    part[x] = acc

    @pl.when(x < 3)
    def _():
        pl.semaphore_wait(ready_far.at[0], 3 - x)

    for k in range(1, 4):
        part_copy(k).start()
    for k in range(1, 4):
        part_copy(k).wait_recv()
    acc = part[0]
    for k in range(1, 4):
        acc = merge(acc, part[k], lane)
    half[high_z] = acc

    @pl.when(high_z == 0)
    def _():
        pl.semaphore_wait(ready_far.at[1], 1)

    half_copy.start()
    half_copy.wait_recv()
    acc = merge(half[0], half[1], lane)

    low, high, valid = acc[:, 0:1], acc[:, 1:2], acc[:, 2:3]
    divisor = jnp.maximum(valid, 1.0)
    average = acc[:, 3:4] / divisor
    variance = acc[:, 4:5] / divisor - average * average
    deviation = jnp.sqrt(jnp.maximum(variance, 0.25))
    table = jnp.where(lane == 0, low, jnp.where(lane == 1, high, jnp.where(
        lane == 2, valid / CELLS, jnp.where(lane == 3, average, deviation))))
    header[...] = table[:BANDS, :5]

    half_copy.wait_send()
    for k in range(1, 4):
        part_copy(k).wait_send()
    for i in range(15):
        piece(i).wait_send()
    for code in range(1, GROUP):
        stat_copy(code, pos).wait_send()
        arrived(moved(pos, code)).wait_recv()


def place(tile, header, tile_out, header_out, sems):
    rows = HALF // PARTS
    copies = [pltpu.make_async_copy(header, header_out, sems.at[PARTS])] + [
        pltpu.make_async_copy(tile.at[pl.ds(rows * n, rows)], tile_out.at[pl.ds(rows * n, rows)], sems.at[n])
        for n in range(PARTS)
    ]
    for copy in copies:
        copy.start()
    for copy in copies:
        copy.wait()


def on_device(pixels, valid_flags):
    dma = pltpu.SemaphoreType.DMA
    shapes = (
        jax.ShapeDtypeStruct((HALF, WIDE), jnp.float32),
        jax.ShapeDtypeStruct((BANDS, 5), jnp.float32),
    )
    tile, header = pl.pallas_call(
        kernel,
        out_shape=shapes,
        in_specs=[pl.BlockSpec(memory_space=pltpu.HBM)] * 2,
        out_specs=(pl.BlockSpec(memory_space=pltpu.VMEM), pl.BlockSpec(memory_space=pltpu.VMEM)),
        scratch_shapes=[
            pltpu.VMEM((GROUP, BANDS, STRIP, TILE), jnp.float32),
            pltpu.VMEM((GROUP, BANDS, STRIP, TILE), jnp.int32),
            pltpu.VMEM((GROUP - 1, STRIP, WIDE), jnp.float32),
            pltpu.VMEM((GROUP, 8, LANES), jnp.float32),
            pltpu.VMEM((4, 8, LANES), jnp.float32),
            pltpu.VMEM((2, 8, LANES), jnp.float32),
            dma((2, GROUP)), dma((GROUP - 1,)), dma((GROUP,)),
            dma((GROUP,)), dma((GROUP,)), dma((4,)), dma((4,)), dma, dma,
            pltpu.SemaphoreType.REGULAR((2,)),
        ],
        compiler_params=pltpu.CompilerParams(
            collective_id=0, has_side_effects=True, vmem_limit_bytes=16 * 1024 * 1024),
        name="export",
    )(
        pltpu.with_memory_space_constraint(pixels, pltpu.HBM),
        pltpu.with_memory_space_constraint(valid_flags, pltpu.HBM),
    )
    tile, header = pl.pallas_call(
        place,
        out_shape=shapes,
        in_specs=[pl.BlockSpec(memory_space=pltpu.VMEM)] * 2,
        out_specs=(pl.BlockSpec(memory_space=pltpu.HBM), pl.BlockSpec(memory_space=pltpu.HBM)),
        scratch_shapes=[dma((PARTS + 1,))],
        compiler_params=pltpu.CompilerParams(vmem_limit_bytes=16 * 1024 * 1024),
        name="place",
    )(tile, header)
    return tile.reshape(1, HALF, WIDE), header.T


def solution(mesh):
    placed = (P(None, "dev", None), P(None, "dev", None))
    return jax.shard_map(
        on_device, mesh=mesh, in_specs=placed, out_specs=(P("dev", None, None), P()), check_vma=False
    )
```

```python
import jax
import jax.numpy as jnp
from jax import lax
from jax.experimental import pallas as pl
from jax.experimental.pallas import tpu as pltpu
from jax.sharding import PartitionSpec as P

BANDS = 4
TILE = 512
STRIP = 16
GROUP = 16
HALF = 256
WIDE = TILE * BANDS
CELLS = 16777216.0
LARGEST = 3e38
LANES = 128
EARLY = 2
LOADS = 2
PARTS = 4
MESH = pl.DeviceIdType.MESH

STEPS = (
    (12, 2, 9, 13, 5, 10, 6, 14, 11, 7, 15, 3, 1, 4, 8, 0),
    (2, 14, 4, 8, 9, 6, 11, 12, 1, 3, 5, 10, 13, 7, 15, 0),
)

def packed(part):
    value = sum(code << (4 * k) for k, code in enumerate(part))
    return value - (1 << 32) if value >= 1 << 31 else value


WORDS = [(packed(steps[:8]), packed(steps[8:])) for steps in STEPS]


def moved(pos, code):
    return ((pos ^ code) & 9) | ((pos + (code & 6)) & 6)


def merge(a, b, lane):
    return jnp.where(lane == 0, jnp.minimum(a, b), jnp.where(lane == 1, jnp.maximum(a, b), a + b))


def kernel(px_hbm, fl_hbm, out, header, px, fl, send, stat, part, half, in_sem, send_sem, recv_sem,
           s1_send, s1_recv, s2_send, s2_recv, s3_send, s3_recv, ready_far):
    me = lax.axis_index("dev")
    pos = me & 15
    base = me - pos
    x = me >> 5
    high_z = (me >> 4) & 1
    first, second = [jnp.where((me & 1) == 0, even, odd) for even, odd in zip(*WORDS)]

    def target(i):
        return moved(pos, (jnp.where(i < 8, first, second) >> ((i & 7) * 4)) & 15)

    def x_partner(k):
        return (me + 32 * k) & 127

    across = me ^ 24

    def load_px(i):
        at = pl.multiple_of(target(i) * TILE, TILE)
        return pltpu.make_async_copy(px_hbm.at[:, :, pl.ds(at, TILE)], px.at[i], in_sem.at[0, i])

    def load_fl(i):
        at = pl.multiple_of(target(i) * TILE, TILE)
        return pltpu.make_async_copy(fl_hbm.at[:, :, pl.ds(at, TILE)], fl.at[i], in_sem.at[1, i])

    barrier = pltpu.get_barrier_semaphore()
    for i in range(LOADS):
        load_px(i).start()
        load_fl(i).start()
    for code in range(1, GROUP):
        pl.semaphore_signal(barrier, inc=1, device_id=(base + moved(pos, code),), device_id_type=MESH)
    for k in range(1, 4):
        @pl.when(x + k < 4)
        def _():
            pl.semaphore_signal(barrier, inc=1, device_id=(x_partner(k),), device_id_type=MESH)

    @pl.when(high_z == 0)
    def _():
        pl.semaphore_signal(barrier, inc=1, device_id=(across,), device_id_type=MESH)

    for i in range(LOADS, GROUP):
        load_px(i).start()
        load_fl(i).start()

    def enter():
        pl.semaphore_wait(barrier, 15 + x + high_z)
        for k in range(1, 4):
            @pl.when(x + k >= 4)
            def _():
                pl.semaphore_signal(ready_far.at[0], inc=1, device_id=(x_partner(k),), device_id_type=MESH)

        @pl.when(high_z == 1)
        def _():
            pl.semaphore_signal(ready_far.at[1], inc=1, device_id=(across,), device_id_type=MESH)

    my_rows = pl.multiple_of(pos * STRIP, STRIP)

    def piece(i):
        return pltpu.make_async_remote_copy(
            src_ref=send.at[i], dst_ref=out.at[pl.ds(my_rows, STRIP)],
            send_sem=send_sem.at[i], recv_sem=recv_sem.at[pos],
            device_id=(base + target(i),), device_id_type=MESH)

    def arrived(source):
        return pltpu.make_async_remote_copy(
            src_ref=send.at[0], dst_ref=out.at[pl.ds(my_rows, STRIP)],
            send_sem=send_sem.at[0], recv_sem=recv_sem.at[source],
            device_id=(base + source,), device_id_type=MESH)

    def stat_copy(code, slot):
        return pltpu.make_async_remote_copy(
            src_ref=stat.at[pos], dst_ref=stat.at[pos],
            send_sem=s1_send.at[code], recv_sem=s1_recv.at[slot],
            device_id=(base + moved(pos, code),), device_id_type=MESH)

    def part_copy(k):
        return pltpu.make_async_remote_copy(
            src_ref=part.at[x], dst_ref=part.at[x],
            send_sem=s2_send.at[k], recv_sem=s2_recv.at[k],
            device_id=(x_partner(k),), device_id_type=MESH)

    half_copy = pltpu.make_async_remote_copy(
        src_ref=half.at[high_z], dst_ref=half.at[high_z], send_sem=s3_send, recv_sem=s3_recv,
        device_id=(across,), device_id_type=MESH)

    lane = lax.broadcasted_iota(jnp.int32, (8, LANES), 1)
    row = lax.broadcasted_iota(jnp.int32, (8, LANES), 0)
    block = lane // 32
    order = [((q + lane % 4) % 4) * 32 + lane // 4 for q in range(4)]

    def work(i, carry, store):
        load_px(i).wait()
        load_fl(i).wait()
        low, high, count, summed, square = [list(part) for part in carry]
        sums = [[] for _ in range(BANDS)]
        squares = [[] for _ in range(BANDS)]
        for r in range(2):
            for j in range(4):
                turned = []
                for b in range(BANDS):
                    value = px[i, b, pl.ds(8 * r, 8), pl.ds(LANES * j, LANES)]
                    flag = fl[i, b, pl.ds(8 * r, 8), pl.ds(LANES * j, LANES)]
                    usable = flag == 1
                    filled = jnp.where(usable, value, 0.0)
                    low[b] = jnp.minimum(low[b], jnp.where(usable, value, LARGEST))
                    high[b] = jnp.maximum(high[b], jnp.where(usable, value, -LARGEST))
                    count[b] = count[b] + flag
                    sums[b].append(filled)
                    squares[b].append(filled * filled)
                    turned.append(filled if b == 0 else pltpu.roll(filled, 32 * b, 1))
                for q in range(4):
                    mixed = turned[(0 - q) % 4]
                    for k in range(1, 4):
                        mixed = jnp.where(block == k, turned[(k - q) % 4], mixed)
                    store(r, j * 4 + q, jnp.take_along_axis(mixed, order[q], axis=1))

        def tree(parts):
            while len(parts) > 1:
                parts = [a + b for a, b in zip(parts[::2], parts[1::2])]
            return parts[0]

        for b in range(BANDS):
            summed[b] = summed[b] + tree(sums[b])
            square[b] = square[b] + tree(squares[b])
        return tuple(tuple(part) for part in (low, high, count, summed, square))

    zero = jnp.zeros((8, LANES), jnp.float32)
    carry = (
        (zero + LARGEST,) * BANDS, (zero - LARGEST,) * BANDS,
        (jnp.zeros((8, LANES), jnp.int32),) * BANDS, (zero,) * BANDS, (zero,) * BANDS,
    )

    def step(i, carry):
        def store(r, c, value):
            send[i, pl.ds(8 * r, 8), pl.ds(LANES * c, LANES)] = value

        carry = work(i, carry, store)

        @pl.when(i == 0)
        def _():
            enter()

        @pl.when(i < EARLY)
        def _():
            piece(i).start()

        return carry

    carry = lax.fori_loop(0, 15, step, carry)

    def store_own(r, c, value):
        out[pl.ds(pl.multiple_of(my_rows + 8 * r, 8), 8), pl.ds(LANES * c, LANES)] = value

    low, high, count, summed, square = work(15, carry, store_own)

    stats = zero
    for b in range(BANDS):
        for s, value in enumerate((
            jnp.min(low[b], axis=(0, 1), keepdims=True),
            jnp.max(high[b], axis=(0, 1), keepdims=True),
            jnp.sum(count[b].astype(jnp.float32), axis=(0, 1), keepdims=True),
            jnp.sum(summed[b], axis=(0, 1), keepdims=True),
            jnp.sum(square[b], axis=(0, 1), keepdims=True),
        )):
            stats = jnp.where((row == b) & (lane == s), value, stats)
    stat[pos] = stats

    for code in reversed(range(1, GROUP)):
        stat_copy(code, pos).start()
    for i in range(EARLY, 15):
        piece(i).start()

    for code in range(1, GROUP):
        stat_copy(code, moved(pos, code)).wait_recv()
    acc = stat[0]
    for k in range(1, GROUP):
        acc = merge(acc, stat[k], lane)
    part[x] = acc

    @pl.when(x < 3)
    def _():
        pl.semaphore_wait(ready_far.at[0], 3 - x)

    for k in range(1, 4):
        part_copy(k).start()
    for k in range(1, 4):
        part_copy(k).wait_recv()
    acc = part[0]
    for k in range(1, 4):
        acc = merge(acc, part[k], lane)
    half[high_z] = acc

    @pl.when(high_z == 0)
    def _():
        pl.semaphore_wait(ready_far.at[1], 1)

    half_copy.start()
    half_copy.wait_recv()
    acc = merge(half[0], half[1], lane)

    low, high, valid = acc[:, 0:1], acc[:, 1:2], acc[:, 2:3]
    divisor = jnp.maximum(valid, 1.0)
    average = acc[:, 3:4] / divisor
    variance = acc[:, 4:5] / divisor - average * average
    deviation = jnp.sqrt(jnp.maximum(variance, 0.25))
    table = jnp.where(lane == 0, low, jnp.where(lane == 1, high, jnp.where(
        lane == 2, valid / CELLS, jnp.where(lane == 3, average, deviation))))
    header[...] = table[:BANDS, :5]

    half_copy.wait_send()
    for k in range(1, 4):
        part_copy(k).wait_send()
    for i in range(15):
        piece(i).wait_send()
    for code in range(1, GROUP):
        stat_copy(code, pos).wait_send()
        arrived(moved(pos, code)).wait_recv()


def place(tile, header, tile_out, header_out, sems):
    rows = HALF // PARTS
    copies = [pltpu.make_async_copy(header, header_out, sems.at[PARTS])] + [
        pltpu.make_async_copy(tile.at[pl.ds(rows * n, rows)], tile_out.at[pl.ds(rows * n, rows)], sems.at[n])
        for n in range(PARTS)
    ]
    for copy in copies:
        copy.start()
    for copy in copies:
        copy.wait()


def on_device(pixels, valid_flags):
    dma = pltpu.SemaphoreType.DMA
    shapes = (
        jax.ShapeDtypeStruct((HALF, WIDE), jnp.float32),
        jax.ShapeDtypeStruct((BANDS, 5), jnp.float32),
    )
    tile, header = pl.pallas_call(
        kernel,
        out_shape=shapes,
        in_specs=[pl.BlockSpec(memory_space=pltpu.HBM)] * 2,
        out_specs=(pl.BlockSpec(memory_space=pltpu.VMEM), pl.BlockSpec(memory_space=pltpu.VMEM)),
        scratch_shapes=[
            pltpu.VMEM((GROUP, BANDS, STRIP, TILE), jnp.float32),
            pltpu.VMEM((GROUP, BANDS, STRIP, TILE), jnp.int32),
            pltpu.VMEM((GROUP - 1, STRIP, WIDE), jnp.float32),
            pltpu.VMEM((GROUP, 8, LANES), jnp.float32),
            pltpu.VMEM((4, 8, LANES), jnp.float32),
            pltpu.VMEM((2, 8, LANES), jnp.float32),
            dma((2, GROUP)), dma((GROUP - 1,)), dma((GROUP,)),
            dma((GROUP,)), dma((GROUP,)), dma((4,)), dma((4,)), dma, dma,
            pltpu.SemaphoreType.REGULAR((2,)),
        ],
        compiler_params=pltpu.CompilerParams(
            collective_id=0, has_side_effects=True, vmem_limit_bytes=16 * 1024 * 1024),
        name="export",
    )(
        pltpu.with_memory_space_constraint(pixels, pltpu.HBM),
        pltpu.with_memory_space_constraint(valid_flags, pltpu.HBM),
    )
    tile, header = pl.pallas_call(
        place,
        out_shape=shapes,
        in_specs=[pl.BlockSpec(memory_space=pltpu.VMEM)] * 2,
        out_specs=(pl.BlockSpec(memory_space=pltpu.HBM), pl.BlockSpec(memory_space=pltpu.HBM)),
        scratch_shapes=[dma((PARTS + 1,))],
        compiler_params=pltpu.CompilerParams(vmem_limit_bytes=16 * 1024 * 1024),
        name="place",
    )(tile, header)
    return tile.reshape(1, HALF, WIDE), header.T


def solution(mesh):
    placed = (P(None, "dev", None), P(None, "dev", None))
    return jax.shard_map(
        on_device, mesh=mesh, in_specs=placed, out_specs=(P("dev", None, None), P()), check_vma=False
    )
```

```python
import jax
import jax.numpy as jnp
from jax import lax
from jax.experimental import pallas as pl
from jax.experimental.pallas import tpu as pltpu
from jax.sharding import PartitionSpec as P

BANDS = 4
TILE = 512
STRIP = 16
GROUP = 16
HALF = 256
WIDE = TILE * BANDS
CELLS = 16777216.0
LARGEST = 3e38
LANES = 128
EARLY = 2
LOADS = 2
PARTS = 4
MESH = pl.DeviceIdType.MESH

STEPS = (
    (12, 2, 9, 13, 5, 10, 6, 14, 11, 7, 15, 3, 1, 4, 8, 0),
    (2, 14, 4, 8, 9, 6, 11, 12, 1, 3, 5, 10, 13, 7, 15, 0),
)

def packed(part):
    value = sum(code << (4 * k) for k, code in enumerate(part))
    return value - (1 << 32) if value >= 1 << 31 else value


WORDS = [(packed(steps[:8]), packed(steps[8:])) for steps in STEPS]


def moved(pos, code):
    return ((pos ^ code) & 9) | ((pos + (code & 6)) & 6)


def merge(a, b, lane):
    return jnp.where(lane == 0, jnp.minimum(a, b), jnp.where(lane == 1, jnp.maximum(a, b), a + b))


def kernel(px_hbm, fl_hbm, out, header, px, fl, send, stat, part, half, in_sem, piece_sem, stat_sem,
           part_sem, half_sem, ready_far):
    me = lax.axis_index("dev")
    pos = me & 15
    base = me - pos
    x = me >> 5
    high_z = (me >> 4) & 1
    first, second = [jnp.where((me & 1) == 0, even, odd) for even, odd in zip(*WORDS)]

    def target(i):
        return moved(pos, (jnp.where(i < 8, first, second) >> ((i & 7) * 4)) & 15)

    def x_partner(k):
        return (me + 32 * k) & 127

    across = me ^ 24

    def load_px(i):
        at = pl.multiple_of(target(i) * TILE, TILE)
        return pltpu.make_async_copy(px_hbm.at[:, :, pl.ds(at, TILE)], px.at[i], in_sem.at[i])

    def load_fl(i):
        at = pl.multiple_of(target(i) * TILE, TILE)
        return pltpu.make_async_copy(fl_hbm.at[:, :, pl.ds(at, TILE)], fl.at[i], in_sem.at[i])

    barrier = pltpu.get_barrier_semaphore()
    for i in range(LOADS):
        load_px(i).start()
        load_fl(i).start()
    for code in range(1, GROUP):
        pl.semaphore_signal(barrier, inc=1, device_id=(base + moved(pos, code),), device_id_type=MESH)
    for k in range(1, 4):
        @pl.when(x + k < 4)
        def _():
            pl.semaphore_signal(barrier, inc=1, device_id=(x_partner(k),), device_id_type=MESH)

    @pl.when(high_z == 0)
    def _():
        pl.semaphore_signal(barrier, inc=1, device_id=(across,), device_id_type=MESH)

    for i in range(LOADS, GROUP):
        load_px(i).start()
        load_fl(i).start()

    def enter():
        pl.semaphore_wait(barrier, 15 + x + high_z)
        for k in range(1, 4):
            @pl.when(x + k >= 4)
            def _():
                pl.semaphore_signal(ready_far.at[0], inc=1, device_id=(x_partner(k),), device_id_type=MESH)

        @pl.when(high_z == 1)
        def _():
            pl.semaphore_signal(ready_far.at[1], inc=1, device_id=(across,), device_id_type=MESH)

    my_rows = pl.multiple_of(pos * STRIP, STRIP)

    def remote(src, dst, sems, there):
        return pltpu.make_async_remote_copy(
            src_ref=src, dst_ref=dst, send_sem=sems.at[0], recv_sem=sems.at[1], device_id=(there,), device_id_type=MESH)

    def piece(i):
        return remote(send.at[i], out.at[pl.ds(my_rows, STRIP)], piece_sem, base + target(i))

    def stat_copy(code):
        return remote(stat.at[pos], stat.at[pos], stat_sem, base + moved(pos, code))

    def part_copy(k):
        return remote(part.at[x], part.at[x], part_sem, x_partner(k))

    all_pieces = remote(out.at[pl.ds(0, HALF - STRIP)], out.at[pl.ds(0, HALF - STRIP)], piece_sem, across)
    all_stats = remote(stat.at[pl.ds(0, GROUP - 1)], stat.at[pl.ds(0, GROUP - 1)], stat_sem, across)
    all_parts = remote(part.at[pl.ds(0, 3)], part.at[pl.ds(0, 3)], part_sem, across)
    half_copy = remote(half.at[high_z], half.at[high_z], half_sem, across)

    lane = lax.broadcasted_iota(jnp.int32, (8, LANES), 1)
    row = lax.broadcasted_iota(jnp.int32, (8, LANES), 0)
    block = lane // 32
    order = [((q + lane % 4) % 4) * 32 + lane // 4 for q in range(4)]

    def work(i, carry, store):
        pltpu.make_async_copy(px.at[pl.ds(0, 2)], px.at[pl.ds(0, 2)], in_sem.at[i]).wait()
        low, high, count, summed, square = [list(part) for part in carry]
        sums = [[] for _ in range(BANDS)]
        squares = [[] for _ in range(BANDS)]
        for r in range(2):
            for j in range(4):
                turned = []
                for b in range(BANDS):
                    value = px[i, b, pl.ds(8 * r, 8), pl.ds(LANES * j, LANES)]
                    flag = fl[i, b, pl.ds(8 * r, 8), pl.ds(LANES * j, LANES)]
                    usable = flag == 1
                    filled = jnp.where(usable, value, 0.0)
                    low[b] = jnp.minimum(low[b], jnp.where(usable, value, LARGEST))
                    high[b] = jnp.maximum(high[b], jnp.where(usable, value, -LARGEST))
                    count[b] = count[b] + flag
                    sums[b].append(filled)
                    squares[b].append(filled * filled)
                    turned.append(filled if b == 0 else pltpu.roll(filled, 32 * b, 1))
                for q in range(4):
                    mixed = turned[(0 - q) % 4]
                    for k in range(1, 4):
                        mixed = jnp.where(block == k, turned[(k - q) % 4], mixed)
                    store(r, j * 4 + q, jnp.take_along_axis(mixed, order[q], axis=1))

        def tree(parts):
            while len(parts) > 1:
                parts = [a + b for a, b in zip(parts[::2], parts[1::2])]
            return parts[0]

        for b in range(BANDS):
            summed[b] = summed[b] + tree(sums[b])
            square[b] = square[b] + tree(squares[b])
        return tuple(tuple(part) for part in (low, high, count, summed, square))

    zero = jnp.zeros((8, LANES), jnp.float32)
    carry = (
        (zero + LARGEST,) * BANDS, (zero - LARGEST,) * BANDS,
        (jnp.zeros((8, LANES), jnp.int32),) * BANDS, (zero,) * BANDS, (zero,) * BANDS,
    )

    def step(i, carry):
        def store(r, c, value):
            send[i, pl.ds(8 * r, 8), pl.ds(LANES * c, LANES)] = value

        carry = work(i, carry, store)

        @pl.when(i == 0)
        def _():
            enter()

        @pl.when(i < EARLY)
        def _():
            piece(i).start()

        return carry

    carry = lax.fori_loop(0, 15, step, carry)

    def store_own(r, c, value):
        out[pl.ds(pl.multiple_of(my_rows + 8 * r, 8), 8), pl.ds(LANES * c, LANES)] = value

    low, high, count, summed, square = work(15, carry, store_own)

    stats = zero
    for b in range(BANDS):
        for s, value in enumerate((
            jnp.min(low[b], axis=(0, 1), keepdims=True),
            jnp.max(high[b], axis=(0, 1), keepdims=True),
            jnp.sum(count[b].astype(jnp.float32), axis=(0, 1), keepdims=True),
            jnp.sum(summed[b], axis=(0, 1), keepdims=True),
            jnp.sum(square[b], axis=(0, 1), keepdims=True),
        )):
            stats = jnp.where((row == b) & (lane == s), value, stats)
    stat[pos] = stats

    for code in reversed(range(1, GROUP)):
        stat_copy(code).start()
    for i in range(EARLY, 15):
        piece(i).start()

    all_stats.wait_recv()
    acc = stat[0]
    for k in range(1, GROUP):
        acc = merge(acc, stat[k], lane)
    part[x] = acc

    @pl.when(x < 3)
    def _():
        pl.semaphore_wait(ready_far.at[0], 3 - x)

    for k in range(1, 4):
        part_copy(k).start()
    all_parts.wait_recv()
    acc = part[0]
    for k in range(1, 4):
        acc = merge(acc, part[k], lane)
    half[high_z] = acc

    @pl.when(high_z == 0)
    def _():
        pl.semaphore_wait(ready_far.at[1], 1)

    half_copy.start()
    half_copy.wait_recv()
    acc = merge(half[0], half[1], lane)

    low, high, valid = acc[:, 0:1], acc[:, 1:2], acc[:, 2:3]
    divisor = jnp.maximum(valid, 1.0)
    average = acc[:, 3:4] / divisor
    variance = acc[:, 4:5] / divisor - average * average
    deviation = jnp.sqrt(jnp.maximum(variance, 0.25))
    table = jnp.where(lane == 0, low, jnp.where(lane == 1, high, jnp.where(
        lane == 2, valid / CELLS, jnp.where(lane == 3, average, deviation))))
    header[...] = table[:BANDS, :5]

    half_copy.wait_send()
    all_parts.wait_send()
    all_stats.wait_send()
    all_pieces.wait_send()
    all_pieces.wait_recv()


def place(tile, header, tile_out, header_out, sems):
    rows = HALF // PARTS
    copies = [pltpu.make_async_copy(header, header_out, sems.at[PARTS])] + [
        pltpu.make_async_copy(tile.at[pl.ds(rows * n, rows)], tile_out.at[pl.ds(rows * n, rows)], sems.at[n])
        for n in range(PARTS)
    ]
    for copy in copies:
        copy.start()
    for copy in copies:
        copy.wait()


def on_device(pixels, valid_flags):
    dma = pltpu.SemaphoreType.DMA
    shapes = (
        jax.ShapeDtypeStruct((HALF, WIDE), jnp.float32),
        jax.ShapeDtypeStruct((BANDS, 5), jnp.float32),
    )
    tile, header = pl.pallas_call(
        kernel,
        out_shape=shapes,
        in_specs=[pl.BlockSpec(memory_space=pltpu.HBM)] * 2,
        out_specs=(pl.BlockSpec(memory_space=pltpu.VMEM), pl.BlockSpec(memory_space=pltpu.VMEM)),
        scratch_shapes=[
            pltpu.VMEM((GROUP, BANDS, STRIP, TILE), jnp.float32),
            pltpu.VMEM((GROUP, BANDS, STRIP, TILE), jnp.int32),
            pltpu.VMEM((GROUP - 1, STRIP, WIDE), jnp.float32),
            pltpu.VMEM((GROUP, 8, LANES), jnp.float32),
            pltpu.VMEM((4, 8, LANES), jnp.float32),
            pltpu.VMEM((2, 8, LANES), jnp.float32),
            dma((GROUP,)), dma((2,)), dma((2,)), dma((2,)), dma((2,)),
            pltpu.SemaphoreType.REGULAR((2,)),
        ],
        compiler_params=pltpu.CompilerParams(
            collective_id=0, has_side_effects=True, vmem_limit_bytes=16 * 1024 * 1024),
        name="export",
    )(
        pltpu.with_memory_space_constraint(pixels, pltpu.HBM),
        pltpu.with_memory_space_constraint(valid_flags, pltpu.HBM),
    )
    tile, header = pl.pallas_call(
        place,
        out_shape=shapes,
        in_specs=[pl.BlockSpec(memory_space=pltpu.VMEM)] * 2,
        out_specs=(pl.BlockSpec(memory_space=pltpu.HBM), pl.BlockSpec(memory_space=pltpu.HBM)),
        scratch_shapes=[dma((PARTS + 1,))],
        compiler_params=pltpu.CompilerParams(vmem_limit_bytes=16 * 1024 * 1024),
        name="place",
    )(tile, header)
    return tile.reshape(1, HALF, WIDE), header.T


def solution(mesh):
    placed = (P(None, "dev", None), P(None, "dev", None))
    return jax.shard_map(
        on_device, mesh=mesh, in_specs=placed, out_specs=(P("dev", None, None), P()), check_vma=False
    )
```

```python
import jax
import jax.numpy as jnp
from jax import lax
from jax.experimental import pallas as pl
from jax.experimental.pallas import tpu as pltpu
from jax.sharding import PartitionSpec as P

BANDS = 4
TILE = 512
STRIP = 16
GROUP = 16
HALF = 256
WIDE = TILE * BANDS
CELLS = 16777216.0
LARGEST = 3e38
LANES = 128
EARLIES = (6, 4)
MIDDLE = 12
SMALL = 7 + 3 + 1 + 1
LOADS = 2
GROUPS = (0, 1, 2, 4, 8)
PARTS = 4
MESH = pl.DeviceIdType.MESH

STEPS = (
    (12, 2, 9, 13, 5, 10, 6, 14, 11, 7, 15, 3, 1, 4, 8, 0),
    (2, 14, 4, 8, 9, 6, 11, 12, 1, 3, 5, 10, 13, 7, 15, 0),
)

def packed(part):
    value = sum(code << (4 * k) for k, code in enumerate(part))
    return value - (1 << 32) if value >= 1 << 31 else value


WORDS = [(packed(steps[:8]), packed(steps[8:])) for steps in STEPS]


def moved(pos, code):
    return ((pos ^ code) & 9) | ((pos + (code & 6)) & 6)


def merge(a, b, lane):
    return jnp.where(lane == 0, jnp.minimum(a, b), jnp.where(lane == 1, jnp.maximum(a, b), a + b))


def kernel(px_hbm, fl_hbm, out, header, px, fl, send, own, pair, stat, part, half, final, in_sem, piece_sem, small_sent, small_got,
           ready_far):
    me = lax.axis_index("dev")
    pos = me & 15
    base = me - pos
    core = me & 1
    chip = pos >> 1
    x = me >> 5
    high_z = (me >> 4) & 1
    first, second = [jnp.where((me & 1) == 0, even, odd) for even, odd in zip(*WORDS)]

    def target(i):
        return moved(pos, (jnp.where(i < 8, first, second) >> ((i & 7) * 4)) & 15)

    def x_partner(k):
        return (me + 32 * k) & 127

    across = me ^ 24

    def start_load(i):
        at = pl.multiple_of(target(i) * TILE, TILE)
        own = in_sem.at[max(g for g, start in enumerate(GROUPS) if start <= i)]
        pltpu.make_async_copy(px_hbm.at[:, :, pl.ds(at, TILE)], px.at[i], own).start()
        pltpu.make_async_copy(fl_hbm.at[:, :, pl.ds(at, TILE)], fl.at[i], own).start()

    barrier = pltpu.get_barrier_semaphore()
    for i in range(LOADS):
        start_load(i)
    for code in range(1, GROUP):
        pl.semaphore_signal(barrier, inc=1, device_id=(base + moved(pos, code),), device_id_type=MESH)
    for k in range(1, 4):
        @pl.when((core == 1) & (x + k < 4))
        def _():
            pl.semaphore_signal(barrier, inc=1, device_id=(x_partner(k),), device_id_type=MESH)

    @pl.when((core == 1) & (high_z == 0))
    def _():
        pl.semaphore_signal(barrier, inc=1, device_id=(across,), device_id_type=MESH)

    for i in range(LOADS, GROUP):
        start_load(i)

    def enter():
        pl.semaphore_wait(barrier, 15 + core * (x + high_z))
        for k in range(1, 4):
            @pl.when((core == 1) & (x + k >= 4))
            def _():
                pl.semaphore_signal(ready_far.at[0], inc=1, device_id=(x_partner(k),), device_id_type=MESH)

        @pl.when((core == 1) & (high_z == 1))
        def _():
            pl.semaphore_signal(ready_far.at[1], inc=1, device_id=(across,), device_id_type=MESH)

    my_rows = pl.multiple_of(pos * STRIP, STRIP)

    def remote(src, dst, sent, got, there):
        return pltpu.make_async_remote_copy(
            src_ref=src, dst_ref=dst, send_sem=sent, recv_sem=got, device_id=(there,), device_id_type=MESH)

    def piece(i):
        return remote(send.at[i], out.at[pl.ds(my_rows, STRIP)], piece_sem.at[0], piece_sem.at[1],
                      base + target(i))

    def stat_copy(code):
        return remote(stat.at[chip], stat.at[chip], small_sent, small_got.at[0], base + moved(pos, code))

    def part_copy(k):
        return remote(part.at[x], part.at[x], small_sent, small_got.at[1], x_partner(k))

    most = out.at[pl.ds(0, HALF - STRIP)]
    all_pieces = remote(most, most, piece_sem.at[0], piece_sem.at[1], across)
    all_stats = remote(stat.at[pl.ds(0, 7)], stat.at[pl.ds(0, 7)], small_sent, small_got.at[0], across)
    all_parts = remote(part.at[pl.ds(0, 3)], part.at[pl.ds(0, 3)], small_sent, small_got.at[1], across)
    half_copy = remote(half.at[high_z], half.at[high_z], small_sent, small_got.at[2], across)
    pair_copy = remote(own, pair, small_sent, small_got.at[3], me ^ 1)
    final_copy = remote(final, final, small_sent, small_got.at[3], me ^ 1)
    all_small = remote(stat.at[pl.ds(0, SMALL)], stat.at[pl.ds(0, SMALL)], small_sent, small_got.at[0], across)

    lane = lax.broadcasted_iota(jnp.int32, (8, LANES), 1)
    row = lax.broadcasted_iota(jnp.int32, (8, LANES), 0)
    block = lane // 32
    order = [((q + lane % 4) % 4) * 32 + lane // 4 for q in range(4)]

    def work(i, carry, store):
        low, high, count, summed, square = [list(part) for part in carry]
        sums = [[] for _ in range(BANDS)]
        squares = [[] for _ in range(BANDS)]
        for r in range(2):
            for j in range(4):
                turned = []
                for b in range(BANDS):
                    value = px[i, b, pl.ds(8 * r, 8), pl.ds(LANES * j, LANES)]
                    flag = fl[i, b, pl.ds(8 * r, 8), pl.ds(LANES * j, LANES)]
                    usable = flag == 1
                    filled = jnp.where(usable, value, 0.0)
                    low[b] = jnp.minimum(low[b], jnp.where(usable, value, LARGEST))
                    high[b] = jnp.maximum(high[b], jnp.where(usable, value, -LARGEST))
                    count[b] = count[b] + flag
                    sums[b].append(filled)
                    squares[b].append(filled * filled)
                    turned.append(filled if b == 0 else pltpu.roll(filled, 32 * b, 1))
                for q in range(4):
                    mixed = turned[(0 - q) % 4]
                    for k in range(1, 4):
                        mixed = jnp.where(block == k, turned[(k - q) % 4], mixed)
                    store(r, j * 4 + q, jnp.take_along_axis(mixed, order[q], axis=1))

        def tree(parts):
            while len(parts) > 1:
                parts = [a + b for a, b in zip(parts[::2], parts[1::2])]
            return parts[0]

        for b in range(BANDS):
            summed[b] = summed[b] + tree(sums[b])
            square[b] = square[b] + tree(squares[b])
        return tuple(tuple(part) for part in (low, high, count, summed, square))

    zero = jnp.zeros((8, LANES), jnp.float32)
    carry = (
        (zero + LARGEST,) * BANDS, (zero - LARGEST,) * BANDS,
        (jnp.zeros((8, LANES), jnp.int32),) * BANDS, (zero,) * BANDS, (zero,) * BANDS,
    )

    def wait_loads(g):
        size = 2 * ((GROUPS + (GROUP,))[g + 1] - GROUPS[g])
        pltpu.make_async_copy(px.at[pl.ds(0, size)], px.at[pl.ds(0, size)], in_sem.at[g]).wait()

    def step(i, carry):
        for g, start in enumerate(GROUPS):
            @pl.when(i == start)
            def _():
                wait_loads(g)

        def store(r, c, value):
            send[i, pl.ds(8 * r, 8), pl.ds(LANES * c, LANES)] = value

        carry = work(i, carry, store)

        @pl.when(i == 0)
        def _():
            enter()

        @pl.when(i < jnp.where(core == 0, EARLIES[0], EARLIES[1]))
        def _():
            piece(i).start()

        return carry

    carry = lax.fori_loop(0, 15, step, carry)

    def store_own(r, c, value):
        out[pl.ds(pl.multiple_of(my_rows + 8 * r, 8), 8), pl.ds(LANES * c, LANES)] = value

    low, high, count, summed, square = work(15, carry, store_own)

    stats = zero
    for b in range(BANDS):
        for s, value in enumerate((
            jnp.min(low[b], axis=(0, 1), keepdims=True),
            jnp.max(high[b], axis=(0, 1), keepdims=True),
            jnp.sum(count[b].astype(jnp.float32), axis=(0, 1), keepdims=True),
            jnp.sum(summed[b], axis=(0, 1), keepdims=True),
            jnp.sum(square[b], axis=(0, 1), keepdims=True),
        )):
            stats = jnp.where((row == b) & (lane == s), value, stats)
    @pl.when(core == 0)
    def _():
        own[...] = stats
        pair_copy.start()

    @pl.when(core == 1)
    def _():
        pair_copy.wait_recv()
        stat[chip] = merge(pair[...], stats, lane)
        for code in range(14, 0, -2):
            stat_copy(code).start()

    @pl.when(core == 0)
    def _():
        for i in range(EARLIES[0], MIDDLE):
            piece(i).start()

    @pl.when(core == 1)
    def _():
        for i in range(EARLIES[1], MIDDLE):
            piece(i).start()

    @pl.when(core == 1)
    def _():
        all_stats.wait_recv()
        acc = stat[0]
        for k in range(1, 8):
            acc = merge(acc, stat[k], lane)
        part[x] = acc

        @pl.when(x < 3)
        def _():
            pl.semaphore_wait(ready_far.at[0], 3 - x)

        for k in range(1, 4):
            part_copy(k).start()

    for i in range(MIDDLE, 15):
        piece(i).start()

    @pl.when(core == 1)
    def _():
        all_parts.wait_recv()
        acc = part[0]
        for k in range(1, 4):
            acc = merge(acc, part[k], lane)
        half[high_z] = acc

        @pl.when(high_z == 0)
        def _():
            pl.semaphore_wait(ready_far.at[1], 1)

        half_copy.start()
        half_copy.wait_recv()
        final[...] = merge(half[0], half[1], lane)
        final_copy.start()

    @pl.when(core == 0)
    def _():
        final_copy.wait_recv()

    acc = final[...]
    low, high, valid = acc[:, 0:1], acc[:, 1:2], acc[:, 2:3]
    divisor = jnp.maximum(valid, 1.0)
    average = acc[:, 3:4] / divisor
    variance = acc[:, 4:5] / divisor - average * average
    deviation = jnp.sqrt(jnp.maximum(variance, 0.25))
    table = jnp.where(lane == 0, low, jnp.where(lane == 1, high, jnp.where(
        lane == 2, valid / CELLS, jnp.where(lane == 3, average, deviation))))
    header[...] = table[:BANDS, :5]

    @pl.when(core == 0)
    def _():
        pair_copy.wait_send()

    @pl.when(core == 1)
    def _():
        all_small.wait_send()

    all_pieces.wait_send()
    all_pieces.wait_recv()


def place(tile, header, tile_out, header_out, sems):
    rows = HALF // PARTS
    copies = [pltpu.make_async_copy(header, header_out, sems.at[PARTS])] + [
        pltpu.make_async_copy(tile.at[pl.ds(rows * n, rows)], tile_out.at[pl.ds(rows * n, rows)], sems.at[n])
        for n in range(PARTS)
    ]
    for copy in copies:
        copy.start()
    for copy in copies:
        copy.wait()


def on_device(pixels, valid_flags):
    dma = pltpu.SemaphoreType.DMA
    shapes = (
        jax.ShapeDtypeStruct((HALF, WIDE), jnp.float32),
        jax.ShapeDtypeStruct((BANDS, 5), jnp.float32),
    )
    tile, header = pl.pallas_call(
        kernel,
        out_shape=shapes,
        in_specs=[pl.BlockSpec(memory_space=pltpu.HBM)] * 2,
        out_specs=(pl.BlockSpec(memory_space=pltpu.VMEM), pl.BlockSpec(memory_space=pltpu.VMEM)),
        scratch_shapes=[
            pltpu.VMEM((GROUP, BANDS, STRIP, TILE), jnp.float32),
            pltpu.VMEM((GROUP, BANDS, STRIP, TILE), jnp.int32),
            pltpu.VMEM((GROUP - 1, STRIP, WIDE), jnp.float32),
            pltpu.VMEM((8, LANES), jnp.float32),
            pltpu.VMEM((8, LANES), jnp.float32),
            pltpu.VMEM((SMALL, 8, LANES), jnp.float32),
            pltpu.VMEM((4, 8, LANES), jnp.float32),
            pltpu.VMEM((2, 8, LANES), jnp.float32),
            pltpu.VMEM((8, LANES), jnp.float32),
            dma((len(GROUPS),)), dma((2,)), dma, dma((4,)),
            pltpu.SemaphoreType.REGULAR((2,)),
        ],
        compiler_params=pltpu.CompilerParams(
            collective_id=0, has_side_effects=True, vmem_limit_bytes=16 * 1024 * 1024),
        name="export",
    )(
        pltpu.with_memory_space_constraint(pixels, pltpu.HBM),
        pltpu.with_memory_space_constraint(valid_flags, pltpu.HBM),
    )
    tile, header = pl.pallas_call(
        place,
        out_shape=shapes,
        in_specs=[pl.BlockSpec(memory_space=pltpu.VMEM)] * 2,
        out_specs=(pl.BlockSpec(memory_space=pltpu.HBM), pl.BlockSpec(memory_space=pltpu.HBM)),
        scratch_shapes=[dma((PARTS + 1,))],
        compiler_params=pltpu.CompilerParams(vmem_limit_bytes=16 * 1024 * 1024),
        name="place",
    )(tile, header)
    return tile.reshape(1, HALF, WIDE), header.T


def solution(mesh):
    placed = (P(None, "dev", None), P(None, "dev", None))
    return jax.shard_map(
        on_device, mesh=mesh, in_specs=placed, out_specs=(P("dev", None, None), P()), check_vma=False
    )
```

```python
import jax
import jax.numpy as jnp
from jax import lax
from jax.experimental import pallas as pl
from jax.experimental.pallas import tpu as pltpu
from jax.sharding import PartitionSpec as P

BANDS = 4
TILE = 512
STRIP = 16
GROUP = 16
HALF = 256
WIDE = TILE * BANDS
CELLS = 16777216.0
LARGEST = 3e38
LANES = 128
EARLIES = (6, 4)
MIDDLE = 12
SMALL = 7 + 3 + 1 + 1
LOADS = 2
GROUPS = (0, 1, 2, 4, 8)
PARTS = 4
MESH = pl.DeviceIdType.MESH

STEPS = (
    (12, 9, 13, 5, 10, 6, 1, 11, 7, 15, 3, 14, 4, 8, 2, 0),
    (2, 14, 8, 4, 9, 6, 11, 5, 12, 1, 3, 10, 13, 7, 15, 0),
)

def packed(part):
    value = sum(code << (4 * k) for k, code in enumerate(part))
    return value - (1 << 32) if value >= 1 << 31 else value


WORDS = [(packed(steps[:8]), packed(steps[8:])) for steps in STEPS]


def moved(pos, code):
    return ((pos ^ code) & 9) | ((pos + (code & 6)) & 6)


def merge(a, b, lane):
    return jnp.where(lane == 0, jnp.minimum(a, b), jnp.where(lane == 1, jnp.maximum(a, b), a + b))


def kernel(px_hbm, fl_hbm, out, header, px, fl, send, own, pair, stat, part, half, final, in_sem, piece_sem, small_sent, small_got,
           ready_far):
    me = lax.axis_index("dev")
    pos = me & 15
    base = me - pos
    core = me & 1
    chip = pos >> 1
    x = me >> 5
    high_z = (me >> 4) & 1
    first, second = [jnp.where((me & 1) == 0, even, odd) for even, odd in zip(*WORDS)]

    def target(i):
        return moved(pos, (jnp.where(i < 8, first, second) >> ((i & 7) * 4)) & 15)

    def x_partner(k):
        return (me + 32 * k) & 127

    across = me ^ 24

    def start_load(i):
        at = pl.multiple_of(target(i) * TILE, TILE)
        own = in_sem.at[max(g for g, start in enumerate(GROUPS) if start <= i)]
        pltpu.make_async_copy(px_hbm.at[:, :, pl.ds(at, TILE)], px.at[i], own).start()
        pltpu.make_async_copy(fl_hbm.at[:, :, pl.ds(at, TILE)], fl.at[i], own).start()

    barrier = pltpu.get_barrier_semaphore()
    for i in range(LOADS):
        start_load(i)
    for code in range(1, GROUP):
        pl.semaphore_signal(barrier, inc=1, device_id=(base + moved(pos, code),), device_id_type=MESH)
    for k in range(1, 4):
        @pl.when((core == 1) & (x + k < 4))
        def _():
            pl.semaphore_signal(barrier, inc=1, device_id=(x_partner(k),), device_id_type=MESH)

    @pl.when((core == 1) & (high_z == 0))
    def _():
        pl.semaphore_signal(barrier, inc=1, device_id=(across,), device_id_type=MESH)

    for i in range(LOADS, GROUP):
        start_load(i)

    def enter():
        pl.semaphore_wait(barrier, 15 + core * (x + high_z))
        for k in range(1, 4):
            @pl.when((core == 1) & (x + k >= 4))
            def _():
                pl.semaphore_signal(ready_far.at[0], inc=1, device_id=(x_partner(k),), device_id_type=MESH)

        @pl.when((core == 1) & (high_z == 1))
        def _():
            pl.semaphore_signal(ready_far.at[1], inc=1, device_id=(across,), device_id_type=MESH)

    my_rows = pl.multiple_of(pos * STRIP, STRIP)

    def remote(src, dst, sent, got, there):
        return pltpu.make_async_remote_copy(
            src_ref=src, dst_ref=dst, send_sem=sent, recv_sem=got, device_id=(there,), device_id_type=MESH)

    def piece(i):
        return remote(send.at[i], out.at[pl.ds(my_rows, STRIP)], piece_sem.at[0], piece_sem.at[1],
                      base + target(i))

    def stat_copy(code):
        return remote(stat.at[chip], stat.at[chip], small_sent, small_got.at[0], base + moved(pos, code))

    def part_copy(k):
        return remote(part.at[x], part.at[x], small_sent, small_got.at[1], x_partner(k))

    most = out.at[pl.ds(0, HALF - STRIP)]
    all_pieces = remote(most, most, piece_sem.at[0], piece_sem.at[1], across)
    all_stats = remote(stat.at[pl.ds(0, 7)], stat.at[pl.ds(0, 7)], small_sent, small_got.at[0], across)
    all_parts = remote(part.at[pl.ds(0, 3)], part.at[pl.ds(0, 3)], small_sent, small_got.at[1], across)
    half_copy = remote(half.at[high_z], half.at[high_z], small_sent, small_got.at[2], across)
    pair_copy = remote(own, pair, small_sent, small_got.at[3], me ^ 1)
    final_copy = remote(final, final, small_sent, small_got.at[3], me ^ 1)
    all_small = remote(stat.at[pl.ds(0, SMALL)], stat.at[pl.ds(0, SMALL)], small_sent, small_got.at[0], across)

    lane = lax.broadcasted_iota(jnp.int32, (8, LANES), 1)
    row = lax.broadcasted_iota(jnp.int32, (8, LANES), 0)
    block = lane // 32
    order = [((q + lane % 4) % 4) * 32 + lane // 4 for q in range(4)]

    def work(i, carry, store):
        low, high, count, summed, square = [list(part) for part in carry]
        sums = [[] for _ in range(BANDS)]
        squares = [[] for _ in range(BANDS)]
        for r in range(2):
            for j in range(4):
                turned = []
                for b in range(BANDS):
                    value = px[i, b, pl.ds(8 * r, 8), pl.ds(LANES * j, LANES)]
                    flag = fl[i, b, pl.ds(8 * r, 8), pl.ds(LANES * j, LANES)]
                    usable = flag == 1
                    filled = jnp.where(usable, value, 0.0)
                    low[b] = jnp.minimum(low[b], jnp.where(usable, value, LARGEST))
                    high[b] = jnp.maximum(high[b], jnp.where(usable, value, -LARGEST))
                    count[b] = count[b] + flag
                    sums[b].append(filled)
                    squares[b].append(filled * filled)
                    turned.append(filled if b == 0 else pltpu.roll(filled, 32 * b, 1))
                for q in range(4):
                    mixed = turned[(0 - q) % 4]
                    for k in range(1, 4):
                        mixed = jnp.where(block == k, turned[(k - q) % 4], mixed)
                    store(r, j * 4 + q, jnp.take_along_axis(mixed, order[q], axis=1))

        def tree(parts):
            while len(parts) > 1:
                parts = [a + b for a, b in zip(parts[::2], parts[1::2])]
            return parts[0]

        for b in range(BANDS):
            summed[b] = summed[b] + tree(sums[b])
            square[b] = square[b] + tree(squares[b])
        return tuple(tuple(part) for part in (low, high, count, summed, square))

    zero = jnp.zeros((8, LANES), jnp.float32)
    carry = (
        (zero + LARGEST,) * BANDS, (zero - LARGEST,) * BANDS,
        (jnp.zeros((8, LANES), jnp.int32),) * BANDS, (zero,) * BANDS, (zero,) * BANDS,
    )

    def wait_loads(g):
        size = 2 * ((GROUPS + (GROUP,))[g + 1] - GROUPS[g])
        pltpu.make_async_copy(px.at[pl.ds(0, size)], px.at[pl.ds(0, size)], in_sem.at[g]).wait()

    def step(i, carry):
        for g, start in enumerate(GROUPS):
            @pl.when(i == start)
            def _():
                wait_loads(g)

        def store(r, c, value):
            send[i, pl.ds(8 * r, 8), pl.ds(LANES * c, LANES)] = value

        carry = work(i, carry, store)

        @pl.when(i == 0)
        def _():
            enter()

        @pl.when(i < jnp.where(core == 0, EARLIES[0], EARLIES[1]))
        def _():
            piece(i).start()

        return carry

    carry = lax.fori_loop(0, 15, step, carry)

    def store_own(r, c, value):
        out[pl.ds(pl.multiple_of(my_rows + 8 * r, 8), 8), pl.ds(LANES * c, LANES)] = value

    low, high, count, summed, square = work(15, carry, store_own)

    stats = zero
    for b in range(BANDS):
        for s, value in enumerate((
            jnp.min(low[b], axis=(0, 1), keepdims=True),
            jnp.max(high[b], axis=(0, 1), keepdims=True),
            jnp.sum(count[b].astype(jnp.float32), axis=(0, 1), keepdims=True),
            jnp.sum(summed[b], axis=(0, 1), keepdims=True),
            jnp.sum(square[b], axis=(0, 1), keepdims=True),
        )):
            stats = jnp.where((row == b) & (lane == s), value, stats)
    @pl.when(core == 0)
    def _():
        own[...] = stats
        pair_copy.start()

    @pl.when(core == 1)
    def _():
        pair_copy.wait_recv()
        stat[chip] = merge(pair[...], stats, lane)
        for code in range(14, 0, -2):
            stat_copy(code).start()

    @pl.when(core == 0)
    def _():
        for i in range(EARLIES[0], MIDDLE):
            piece(i).start()

    @pl.when(core == 1)
    def _():
        for i in range(EARLIES[1], MIDDLE):
            piece(i).start()

    @pl.when(core == 1)
    def _():
        all_stats.wait_recv()
        acc = stat[0]
        for k in range(1, 8):
            acc = merge(acc, stat[k], lane)
        part[x] = acc

        @pl.when(x < 3)
        def _():
            pl.semaphore_wait(ready_far.at[0], 3 - x)

        for k in range(1, 4):
            part_copy(k).start()

    for i in range(MIDDLE, 15):
        piece(i).start()

    @pl.when(core == 1)
    def _():
        all_parts.wait_recv()
        acc = part[0]
        for k in range(1, 4):
            acc = merge(acc, part[k], lane)
        half[high_z] = acc

        @pl.when(high_z == 0)
        def _():
            pl.semaphore_wait(ready_far.at[1], 1)

        half_copy.start()
        half_copy.wait_recv()
        final[...] = merge(half[0], half[1], lane)
        final_copy.start()

    @pl.when(core == 0)
    def _():
        final_copy.wait_recv()

    acc = final[...]
    low, high, valid = acc[:, 0:1], acc[:, 1:2], acc[:, 2:3]
    divisor = jnp.maximum(valid, 1.0)
    average = acc[:, 3:4] / divisor
    variance = acc[:, 4:5] / divisor - average * average
    deviation = jnp.sqrt(jnp.maximum(variance, 0.25))
    table = jnp.where(lane == 0, low, jnp.where(lane == 1, high, jnp.where(
        lane == 2, valid / CELLS, jnp.where(lane == 3, average, deviation))))
    header[...] = table[:BANDS, :5]

    @pl.when(core == 0)
    def _():
        pair_copy.wait_send()

    @pl.when(core == 1)
    def _():
        all_small.wait_send()

    all_pieces.wait_send()
    all_pieces.wait_recv()


def place(tile, header, tile_out, header_out, sems):
    rows = HALF // PARTS
    copies = [pltpu.make_async_copy(header, header_out, sems.at[PARTS])] + [
        pltpu.make_async_copy(tile.at[pl.ds(rows * n, rows)], tile_out.at[pl.ds(rows * n, rows)], sems.at[n])
        for n in range(PARTS)
    ]
    for copy in copies:
        copy.start()
    for copy in copies:
        copy.wait()


def on_device(pixels, valid_flags):
    dma = pltpu.SemaphoreType.DMA
    shapes = (
        jax.ShapeDtypeStruct((HALF, WIDE), jnp.float32),
        jax.ShapeDtypeStruct((BANDS, 5), jnp.float32),
    )
    tile, header = pl.pallas_call(
        kernel,
        out_shape=shapes,
        in_specs=[pl.BlockSpec(memory_space=pltpu.HBM)] * 2,
        out_specs=(pl.BlockSpec(memory_space=pltpu.VMEM), pl.BlockSpec(memory_space=pltpu.VMEM)),
        scratch_shapes=[
            pltpu.VMEM((GROUP, BANDS, STRIP, TILE), jnp.float32),
            pltpu.VMEM((GROUP, BANDS, STRIP, TILE), jnp.int32),
            pltpu.VMEM((GROUP - 1, STRIP, WIDE), jnp.float32),
            pltpu.VMEM((8, LANES), jnp.float32),
            pltpu.VMEM((8, LANES), jnp.float32),
            pltpu.VMEM((SMALL, 8, LANES), jnp.float32),
            pltpu.VMEM((4, 8, LANES), jnp.float32),
            pltpu.VMEM((2, 8, LANES), jnp.float32),
            pltpu.VMEM((8, LANES), jnp.float32),
            dma((len(GROUPS),)), dma((2,)), dma, dma((4,)),
            pltpu.SemaphoreType.REGULAR((2,)),
        ],
        compiler_params=pltpu.CompilerParams(
            collective_id=0, has_side_effects=True, vmem_limit_bytes=16 * 1024 * 1024),
        name="export",
    )(
        pltpu.with_memory_space_constraint(pixels, pltpu.HBM),
        pltpu.with_memory_space_constraint(valid_flags, pltpu.HBM),
    )
    tile, header = pl.pallas_call(
        place,
        out_shape=shapes,
        in_specs=[pl.BlockSpec(memory_space=pltpu.VMEM)] * 2,
        out_specs=(pl.BlockSpec(memory_space=pltpu.HBM), pl.BlockSpec(memory_space=pltpu.HBM)),
        scratch_shapes=[dma((PARTS + 1,))],
        compiler_params=pltpu.CompilerParams(vmem_limit_bytes=16 * 1024 * 1024),
        name="place",
    )(tile, header)
    return tile.reshape(1, HALF, WIDE), header.T


def solution(mesh):
    placed = (P(None, "dev", None), P(None, "dev", None))
    return jax.shard_map(
        on_device, mesh=mesh, in_specs=placed, out_specs=(P("dev", None, None), P()), check_vma=False
    )
```

```python
import jax
import jax.numpy as jnp
from jax import lax
from jax.experimental import pallas as pl
from jax.experimental.pallas import tpu as pltpu
from jax.sharding import PartitionSpec as P

BANDS = 4
TILE = 512
STRIP = 16
GROUP = 16
HALF = 256
WIDE = TILE * BANDS
CELLS = 16777216.0
LARGEST = 3e38
LANES = 128
EARLIES = (12, 4)
MIDDLE = 12
SMALL = 7 + 3 + 1 + 1
LOADS = 2
GROUPS = (0, 1, 2, 4, 8)
PARTS = 4
MESH = pl.DeviceIdType.MESH

STEPS = (
    (12, 9, 13, 5, 10, 6, 1, 11, 7, 15, 3, 14, 4, 8, 2, 0),
    (2, 14, 8, 4, 9, 6, 11, 5, 12, 1, 3, 10, 13, 7, 15, 0),
)

def packed(part):
    value = sum(code << (4 * k) for k, code in enumerate(part))
    return value - (1 << 32) if value >= 1 << 31 else value


WORDS = [(packed(steps[:8]), packed(steps[8:])) for steps in STEPS]


def moved(pos, code):
    return ((pos ^ code) & 9) | ((pos + (code & 6)) & 6)


def merge(a, b, lane):
    return jnp.where(lane == 0, jnp.minimum(a, b), jnp.where(lane == 1, jnp.maximum(a, b), a + b))


def kernel(px_hbm, fl_hbm, out, header, px, fl, send, own, pair, stat, part, half, final, in_sem, piece_sem, small_sent, small_got,
           ready_far):
    me = lax.axis_index("dev")
    pos = me & 15
    base = me - pos
    core = me & 1
    chip = pos >> 1
    x = me >> 5
    high_z = (me >> 4) & 1
    first, second = [jnp.where((me & 1) == 0, even, odd) for even, odd in zip(*WORDS)]

    def target(i):
        return moved(pos, (jnp.where(i < 8, first, second) >> ((i & 7) * 4)) & 15)

    def x_partner(k):
        return (me + 32 * k) & 127

    across = me ^ 24

    def start_load(i):
        at = pl.multiple_of(target(i) * TILE, TILE)
        own = in_sem.at[max(g for g, start in enumerate(GROUPS) if start <= i)]
        pltpu.make_async_copy(px_hbm.at[:, :, pl.ds(at, TILE)], px.at[i], own).start()
        pltpu.make_async_copy(fl_hbm.at[:, :, pl.ds(at, TILE)], fl.at[i], own).start()

    barrier = pltpu.get_barrier_semaphore()
    for i in range(LOADS):
        start_load(i)
    for code in range(1, GROUP):
        pl.semaphore_signal(barrier, inc=1, device_id=(base + moved(pos, code),), device_id_type=MESH)
    for k in range(1, 4):
        @pl.when((core == 1) & (x + k < 4))
        def _():
            pl.semaphore_signal(barrier, inc=1, device_id=(x_partner(k),), device_id_type=MESH)

    @pl.when((core == 1) & (high_z == 0))
    def _():
        pl.semaphore_signal(barrier, inc=1, device_id=(across,), device_id_type=MESH)

    for i in range(LOADS, GROUP):
        start_load(i)

    def enter():
        pl.semaphore_wait(barrier, 15 + core * (x + high_z))
        for k in range(1, 4):
            @pl.when((core == 1) & (x + k >= 4))
            def _():
                pl.semaphore_signal(ready_far.at[0], inc=1, device_id=(x_partner(k),), device_id_type=MESH)

        @pl.when((core == 1) & (high_z == 1))
        def _():
            pl.semaphore_signal(ready_far.at[1], inc=1, device_id=(across,), device_id_type=MESH)

    my_rows = pl.multiple_of(pos * STRIP, STRIP)

    def remote(src, dst, sent, got, there):
        return pltpu.make_async_remote_copy(
            src_ref=src, dst_ref=dst, send_sem=sent, recv_sem=got, device_id=(there,), device_id_type=MESH)

    def piece(i):
        return remote(send.at[i], out.at[pl.ds(my_rows, STRIP)], piece_sem.at[0], piece_sem.at[1],
                      base + target(i))

    def stat_copy(code):
        return remote(stat.at[chip], stat.at[chip], small_sent, small_got.at[0], base + moved(pos, code))

    def part_copy(k):
        return remote(part.at[x], part.at[x], small_sent, small_got.at[1], x_partner(k))

    most = out.at[pl.ds(0, HALF - STRIP)]
    all_pieces = remote(most, most, piece_sem.at[0], piece_sem.at[1], across)
    all_stats = remote(stat.at[pl.ds(0, 7)], stat.at[pl.ds(0, 7)], small_sent, small_got.at[0], across)
    all_parts = remote(part.at[pl.ds(0, 3)], part.at[pl.ds(0, 3)], small_sent, small_got.at[1], across)
    half_copy = remote(half.at[high_z], half.at[high_z], small_sent, small_got.at[2], across)
    pair_copy = remote(own, pair, small_sent, small_got.at[3], me ^ 1)
    final_copy = remote(final, final, small_sent, small_got.at[3], me ^ 1)
    all_small = remote(stat.at[pl.ds(0, SMALL)], stat.at[pl.ds(0, SMALL)], small_sent, small_got.at[0], across)

    lane = lax.broadcasted_iota(jnp.int32, (8, LANES), 1)
    row = lax.broadcasted_iota(jnp.int32, (8, LANES), 0)
    block = lane // 32
    order = [((q + lane % 4) % 4) * 32 + lane // 4 for q in range(4)]

    def work(i, carry, store):
        low, high, count, summed, square = [list(part) for part in carry]
        sums = [[] for _ in range(BANDS)]
        squares = [[] for _ in range(BANDS)]
        for r in range(2):
            for j in range(4):
                turned = []
                for b in range(BANDS):
                    value = px[i, b, pl.ds(8 * r, 8), pl.ds(LANES * j, LANES)]
                    flag = fl[i, b, pl.ds(8 * r, 8), pl.ds(LANES * j, LANES)]
                    usable = flag == 1
                    filled = jnp.where(usable, value, 0.0)
                    low[b] = jnp.minimum(low[b], jnp.where(usable, value, LARGEST))
                    high[b] = jnp.maximum(high[b], jnp.where(usable, value, -LARGEST))
                    count[b] = count[b] + flag
                    sums[b].append(filled)
                    squares[b].append(filled * filled)
                    turned.append(filled if b == 0 else pltpu.roll(filled, 32 * b, 1))
                for q in range(4):
                    mixed = turned[(0 - q) % 4]
                    for k in range(1, 4):
                        mixed = jnp.where(block == k, turned[(k - q) % 4], mixed)
                    store(r, j * 4 + q, jnp.take_along_axis(mixed, order[q], axis=1))

        def tree(parts):
            while len(parts) > 1:
                parts = [a + b for a, b in zip(parts[::2], parts[1::2])]
            return parts[0]

        for b in range(BANDS):
            summed[b] = summed[b] + tree(sums[b])
            square[b] = square[b] + tree(squares[b])
        return tuple(tuple(part) for part in (low, high, count, summed, square))

    zero = jnp.zeros((8, LANES), jnp.float32)
    carry = (
        (zero + LARGEST,) * BANDS, (zero - LARGEST,) * BANDS,
        (jnp.zeros((8, LANES), jnp.int32),) * BANDS, (zero,) * BANDS, (zero,) * BANDS,
    )

    def wait_loads(g):
        size = 2 * ((GROUPS + (GROUP,))[g + 1] - GROUPS[g])
        pltpu.make_async_copy(px.at[pl.ds(0, size)], px.at[pl.ds(0, size)], in_sem.at[g]).wait()

    def step(i, carry):
        for g, start in enumerate(GROUPS):
            @pl.when(i == start)
            def _():
                wait_loads(g)

        def store(r, c, value):
            send[i, pl.ds(8 * r, 8), pl.ds(LANES * c, LANES)] = value

        carry = work(i, carry, store)

        @pl.when(i == 0)
        def _():
            enter()

        @pl.when(i < jnp.where(core == 0, EARLIES[0], EARLIES[1]))
        def _():
            piece(i).start()

        return carry

    carry = lax.fori_loop(0, 15, step, carry)

    def store_own(r, c, value):
        out[pl.ds(pl.multiple_of(my_rows + 8 * r, 8), 8), pl.ds(LANES * c, LANES)] = value

    low, high, count, summed, square = work(15, carry, store_own)

    stats = zero
    for b in range(BANDS):
        for s, value in enumerate((
            jnp.min(low[b], axis=(0, 1), keepdims=True),
            jnp.max(high[b], axis=(0, 1), keepdims=True),
            jnp.sum(count[b].astype(jnp.float32), axis=(0, 1), keepdims=True),
            jnp.sum(summed[b], axis=(0, 1), keepdims=True),
            jnp.sum(square[b], axis=(0, 1), keepdims=True),
        )):
            stats = jnp.where((row == b) & (lane == s), value, stats)
    @pl.when(core == 0)
    def _():
        own[...] = stats
        pair_copy.start()

    @pl.when(core == 1)
    def _():
        pair_copy.wait_recv()
        stat[chip] = merge(pair[...], stats, lane)
        for code in range(14, 0, -2):
            stat_copy(code).start()

    @pl.when(core == 0)
    def _():
        for i in range(EARLIES[0], MIDDLE):
            piece(i).start()

    @pl.when(core == 1)
    def _():
        for i in range(EARLIES[1], MIDDLE):
            piece(i).start()

    @pl.when(core == 1)
    def _():
        all_stats.wait_recv()
        acc = stat[0]
        for k in range(1, 8):
            acc = merge(acc, stat[k], lane)
        part[x] = acc

        @pl.when(x < 3)
        def _():
            pl.semaphore_wait(ready_far.at[0], 3 - x)

        for k in range(1, 4):
            part_copy(k).start()

    for i in range(MIDDLE, 15):
        piece(i).start()

    @pl.when(core == 1)
    def _():
        all_parts.wait_recv()
        acc = part[0]
        for k in range(1, 4):
            acc = merge(acc, part[k], lane)
        half[high_z] = acc

        @pl.when(high_z == 0)
        def _():
            pl.semaphore_wait(ready_far.at[1], 1)

        half_copy.start()
        half_copy.wait_recv()
        final[...] = merge(half[0], half[1], lane)
        final_copy.start()

    @pl.when(core == 0)
    def _():
        final_copy.wait_recv()

    acc = final[...]
    low, high, valid = acc[:, 0:1], acc[:, 1:2], acc[:, 2:3]
    divisor = jnp.maximum(valid, 1.0)
    average = acc[:, 3:4] / divisor
    variance = acc[:, 4:5] / divisor - average * average
    deviation = jnp.sqrt(jnp.maximum(variance, 0.25))
    table = jnp.where(lane == 0, low, jnp.where(lane == 1, high, jnp.where(
        lane == 2, valid / CELLS, jnp.where(lane == 3, average, deviation))))
    header[...] = table[:BANDS, :5]

    @pl.when(core == 0)
    def _():
        pair_copy.wait_send()

    @pl.when(core == 1)
    def _():
        all_small.wait_send()

    all_pieces.wait_send()
    all_pieces.wait_recv()


def place(tile, header, tile_out, header_out, sems):
    rows = HALF // PARTS
    copies = [pltpu.make_async_copy(header, header_out, sems.at[PARTS])] + [
        pltpu.make_async_copy(tile.at[pl.ds(rows * n, rows)], tile_out.at[pl.ds(rows * n, rows)], sems.at[n])
        for n in range(PARTS)
    ]
    for copy in copies:
        copy.start()
    for copy in copies:
        copy.wait()


def on_device(pixels, valid_flags):
    dma = pltpu.SemaphoreType.DMA
    shapes = (
        jax.ShapeDtypeStruct((HALF, WIDE), jnp.float32),
        jax.ShapeDtypeStruct((BANDS, 5), jnp.float32),
    )
    tile, header = pl.pallas_call(
        kernel,
        out_shape=shapes,
        in_specs=[pl.BlockSpec(memory_space=pltpu.HBM)] * 2,
        out_specs=(pl.BlockSpec(memory_space=pltpu.VMEM), pl.BlockSpec(memory_space=pltpu.VMEM)),
        scratch_shapes=[
            pltpu.VMEM((GROUP, BANDS, STRIP, TILE), jnp.float32),
            pltpu.VMEM((GROUP, BANDS, STRIP, TILE), jnp.int32),
            pltpu.VMEM((GROUP - 1, STRIP, WIDE), jnp.float32),
            pltpu.VMEM((8, LANES), jnp.float32),
            pltpu.VMEM((8, LANES), jnp.float32),
            pltpu.VMEM((SMALL, 8, LANES), jnp.float32),
            pltpu.VMEM((4, 8, LANES), jnp.float32),
            pltpu.VMEM((2, 8, LANES), jnp.float32),
            pltpu.VMEM((8, LANES), jnp.float32),
            dma((len(GROUPS),)), dma((2,)), dma, dma((4,)),
            pltpu.SemaphoreType.REGULAR((2,)),
        ],
        compiler_params=pltpu.CompilerParams(
            collective_id=0, has_side_effects=True, vmem_limit_bytes=16 * 1024 * 1024),
        name="export",
    )(
        pltpu.with_memory_space_constraint(pixels, pltpu.HBM),
        pltpu.with_memory_space_constraint(valid_flags, pltpu.HBM),
    )
    tile, header = pl.pallas_call(
        place,
        out_shape=shapes,
        in_specs=[pl.BlockSpec(memory_space=pltpu.VMEM)] * 2,
        out_specs=(pl.BlockSpec(memory_space=pltpu.HBM), pl.BlockSpec(memory_space=pltpu.HBM)),
        scratch_shapes=[dma((PARTS + 1,))],
        compiler_params=pltpu.CompilerParams(vmem_limit_bytes=16 * 1024 * 1024),
        name="place",
    )(tile, header)
    return tile.reshape(1, HALF, WIDE), header.T


def solution(mesh):
    placed = (P(None, "dev", None), P(None, "dev", None))
    return jax.shard_map(
        on_device, mesh=mesh, in_specs=placed, out_specs=(P("dev", None, None), P()), check_vma=False
    )
```

```python
import jax
import jax.numpy as jnp
from jax import lax
from jax.experimental import pallas as pl
from jax.experimental.pallas import tpu as pltpu
from jax.sharding import PartitionSpec as P

BANDS = 4
TILE = 512
STRIP = 16
GROUP = 16
HALF = 256
WIDE = TILE * BANDS
CELLS = 16777216.0
LARGEST = 3e38
LANES = 128
EARLIES = (6, 4)
MIDDLE = 12
SMALL = 7 + 3 + 1 + 1
LOADS = 2
GROUPS = (0, 1, 2, 4, 8)
PARTS = 4
MESH = pl.DeviceIdType.MESH

STEPS = (
    (12, 13, 9, 5, 11, 6, 1, 10, 7, 15, 14, 3, 4, 8, 2, 0),
    (2, 14, 4, 8, 9, 6, 11, 5, 15, 12, 1, 3, 10, 13, 7, 0),
)

def packed(part):
    value = sum(code << (4 * k) for k, code in enumerate(part))
    return value - (1 << 32) if value >= 1 << 31 else value


WORDS = [(packed(steps[:8]), packed(steps[8:])) for steps in STEPS]


def moved(pos, code):
    return ((pos ^ code) & 9) | ((pos + (code & 6)) & 6)


def merge(a, b, lane):
    return jnp.where(lane == 0, jnp.minimum(a, b), jnp.where(lane == 1, jnp.maximum(a, b), a + b))


def kernel(px_hbm, fl_hbm, out, header, px, fl, send, own, pair, stat, part, half, final, in_sem, piece_sem, small_sent, small_got,
           ready_far):
    me = lax.axis_index("dev")
    pos = me & 15
    base = me - pos
    core = me & 1
    chip = pos >> 1
    x = me >> 5
    high_z = (me >> 4) & 1
    first, second = [jnp.where((me & 1) == 0, even, odd) for even, odd in zip(*WORDS)]

    def target(i):
        return moved(pos, (jnp.where(i < 8, first, second) >> ((i & 7) * 4)) & 15)

    def x_partner(k):
        return (me + 32 * k) & 127

    across = me ^ 24

    def start_load(i):
        at = pl.multiple_of(target(i) * TILE, TILE)
        own = in_sem.at[max(g for g, start in enumerate(GROUPS) if start <= i)]
        pltpu.make_async_copy(px_hbm.at[:, :, pl.ds(at, TILE)], px.at[i], own).start()
        pltpu.make_async_copy(fl_hbm.at[:, :, pl.ds(at, TILE)], fl.at[i], own).start()

    barrier = pltpu.get_barrier_semaphore()
    for i in range(LOADS):
        start_load(i)
    for code in range(1, GROUP):
        pl.semaphore_signal(barrier, inc=1, device_id=(base + moved(pos, code),), device_id_type=MESH)
    for k in range(1, 4):
        @pl.when((core == 1) & (x + k < 4))
        def _():
            pl.semaphore_signal(barrier, inc=1, device_id=(x_partner(k),), device_id_type=MESH)

    @pl.when((core == 1) & (high_z == 0))
    def _():
        pl.semaphore_signal(barrier, inc=1, device_id=(across,), device_id_type=MESH)

    for i in range(LOADS, GROUP):
        start_load(i)

    def enter():
        pl.semaphore_wait(barrier, 15 + core * (x + high_z))
        for k in range(1, 4):
            @pl.when((core == 1) & (x + k >= 4))
            def _():
                pl.semaphore_signal(ready_far.at[0], inc=1, device_id=(x_partner(k),), device_id_type=MESH)

        @pl.when((core == 1) & (high_z == 1))
        def _():
            pl.semaphore_signal(ready_far.at[1], inc=1, device_id=(across,), device_id_type=MESH)

    my_rows = pl.multiple_of(pos * STRIP, STRIP)

    def remote(src, dst, sent, got, there):
        return pltpu.make_async_remote_copy(
            src_ref=src, dst_ref=dst, send_sem=sent, recv_sem=got, device_id=(there,), device_id_type=MESH)

    def piece(i):
        return remote(send.at[i], out.at[pl.ds(my_rows, STRIP)], piece_sem.at[0], piece_sem.at[1],
                      base + target(i))

    def stat_copy(code):
        return remote(stat.at[chip], stat.at[chip], small_sent, small_got.at[0], base + moved(pos, code))

    def part_copy(k):
        return remote(part.at[x], part.at[x], small_sent, small_got.at[1], x_partner(k))

    most = out.at[pl.ds(0, HALF - STRIP)]
    all_pieces = remote(most, most, piece_sem.at[0], piece_sem.at[1], across)
    all_stats = remote(stat.at[pl.ds(0, 7)], stat.at[pl.ds(0, 7)], small_sent, small_got.at[0], across)
    all_parts = remote(part.at[pl.ds(0, 3)], part.at[pl.ds(0, 3)], small_sent, small_got.at[1], across)
    half_copy = remote(half.at[high_z], half.at[high_z], small_sent, small_got.at[2], across)
    pair_copy = remote(own, pair, small_sent, small_got.at[3], me ^ 1)
    final_copy = remote(final, final, small_sent, small_got.at[3], me ^ 1)
    all_small = remote(stat.at[pl.ds(0, SMALL)], stat.at[pl.ds(0, SMALL)], small_sent, small_got.at[0], across)

    lane = lax.broadcasted_iota(jnp.int32, (8, LANES), 1)
    row = lax.broadcasted_iota(jnp.int32, (8, LANES), 0)
    block = lane // 32
    order = [((q + lane % 4) % 4) * 32 + lane // 4 for q in range(4)]

    def work(i, carry, store):
        low, high, count, summed, square = [list(part) for part in carry]
        sums = [[] for _ in range(BANDS)]
        squares = [[] for _ in range(BANDS)]
        for r in range(2):
            for j in range(4):
                turned = []
                for b in range(BANDS):
                    value = px[i, b, pl.ds(8 * r, 8), pl.ds(LANES * j, LANES)]
                    flag = fl[i, b, pl.ds(8 * r, 8), pl.ds(LANES * j, LANES)]
                    usable = flag == 1
                    filled = jnp.where(usable, value, 0.0)
                    low[b] = jnp.minimum(low[b], jnp.where(usable, value, LARGEST))
                    high[b] = jnp.maximum(high[b], jnp.where(usable, value, -LARGEST))
                    count[b] = count[b] + flag
                    sums[b].append(filled)
                    squares[b].append(filled * filled)
                    turned.append(filled if b == 0 else pltpu.roll(filled, 32 * b, 1))
                for q in range(4):
                    mixed = turned[(0 - q) % 4]
                    for k in range(1, 4):
                        mixed = jnp.where(block == k, turned[(k - q) % 4], mixed)
                    store(r, j * 4 + q, jnp.take_along_axis(mixed, order[q], axis=1))

        def tree(parts):
            while len(parts) > 1:
                parts = [a + b for a, b in zip(parts[::2], parts[1::2])]
            return parts[0]

        for b in range(BANDS):
            summed[b] = summed[b] + tree(sums[b])
            square[b] = square[b] + tree(squares[b])
        return tuple(tuple(part) for part in (low, high, count, summed, square))

    zero = jnp.zeros((8, LANES), jnp.float32)
    carry = (
        (zero + LARGEST,) * BANDS, (zero - LARGEST,) * BANDS,
        (jnp.zeros((8, LANES), jnp.int32),) * BANDS, (zero,) * BANDS, (zero,) * BANDS,
    )

    def wait_loads(g):
        size = 2 * ((GROUPS + (GROUP,))[g + 1] - GROUPS[g])
        pltpu.make_async_copy(px.at[pl.ds(0, size)], px.at[pl.ds(0, size)], in_sem.at[g]).wait()

    def step(i, carry):
        for g, start in enumerate(GROUPS):
            @pl.when(i == start)
            def _():
                wait_loads(g)

        def store(r, c, value):
            send[i, pl.ds(8 * r, 8), pl.ds(LANES * c, LANES)] = value

        carry = work(i, carry, store)

        @pl.when(i == 0)
        def _():
            enter()

        @pl.when(i < jnp.where(core == 0, EARLIES[0], EARLIES[1]))
        def _():
            piece(i).start()

        return carry

    carry = lax.fori_loop(0, 15, step, carry)

    def store_own(r, c, value):
        out[pl.ds(pl.multiple_of(my_rows + 8 * r, 8), 8), pl.ds(LANES * c, LANES)] = value

    low, high, count, summed, square = work(15, carry, store_own)

    stats = zero
    for b in range(BANDS):
        for s, value in enumerate((
            jnp.min(low[b], axis=(0, 1), keepdims=True),
            jnp.max(high[b], axis=(0, 1), keepdims=True),
            jnp.sum(count[b].astype(jnp.float32), axis=(0, 1), keepdims=True),
            jnp.sum(summed[b], axis=(0, 1), keepdims=True),
            jnp.sum(square[b], axis=(0, 1), keepdims=True),
        )):
            stats = jnp.where((row == b) & (lane == s), value, stats)
    @pl.when(core == 0)
    def _():
        own[...] = stats
        pair_copy.start()

    @pl.when(core == 1)
    def _():
        pair_copy.wait_recv()
        stat[chip] = merge(pair[...], stats, lane)
        for code in range(14, 0, -2):
            stat_copy(code).start()

    @pl.when(core == 0)
    def _():
        for i in range(EARLIES[0], MIDDLE):
            piece(i).start()

    @pl.when(core == 1)
    def _():
        for i in range(EARLIES[1], MIDDLE):
            piece(i).start()

    @pl.when(core == 1)
    def _():
        all_stats.wait_recv()
        acc = stat[0]
        for k in range(1, 8):
            acc = merge(acc, stat[k], lane)
        part[x] = acc

        @pl.when(x < 3)
        def _():
            pl.semaphore_wait(ready_far.at[0], 3 - x)

        for k in range(1, 4):
            part_copy(k).start()

    for i in range(MIDDLE, 15):
        piece(i).start()

    @pl.when(core == 1)
    def _():
        all_parts.wait_recv()
        acc = part[0]
        for k in range(1, 4):
            acc = merge(acc, part[k], lane)
        half[high_z] = acc

        @pl.when(high_z == 0)
        def _():
            pl.semaphore_wait(ready_far.at[1], 1)

        half_copy.start()
        half_copy.wait_recv()
        final[...] = merge(half[0], half[1], lane)
        final_copy.start()

    @pl.when(core == 0)
    def _():
        final_copy.wait_recv()

    acc = final[...]
    low, high, valid = acc[:, 0:1], acc[:, 1:2], acc[:, 2:3]
    divisor = jnp.maximum(valid, 1.0)
    average = acc[:, 3:4] / divisor
    variance = acc[:, 4:5] / divisor - average * average
    deviation = jnp.sqrt(jnp.maximum(variance, 0.25))
    table = jnp.where(lane == 0, low, jnp.where(lane == 1, high, jnp.where(
        lane == 2, valid / CELLS, jnp.where(lane == 3, average, deviation))))
    header[...] = table[:BANDS, :5]

    @pl.when(core == 0)
    def _():
        pair_copy.wait_send()

    @pl.when(core == 1)
    def _():
        all_small.wait_send()

    all_pieces.wait_send()
    all_pieces.wait_recv()


def place(tile, header, tile_out, header_out, sems):
    rows = HALF // PARTS
    copies = [pltpu.make_async_copy(header, header_out, sems.at[PARTS])] + [
        pltpu.make_async_copy(tile.at[pl.ds(rows * n, rows)], tile_out.at[pl.ds(rows * n, rows)], sems.at[n])
        for n in range(PARTS)
    ]
    for copy in copies:
        copy.start()
    for copy in copies:
        copy.wait()


def on_device(pixels, valid_flags):
    dma = pltpu.SemaphoreType.DMA
    shapes = (
        jax.ShapeDtypeStruct((HALF, WIDE), jnp.float32),
        jax.ShapeDtypeStruct((BANDS, 5), jnp.float32),
    )
    tile, header = pl.pallas_call(
        kernel,
        out_shape=shapes,
        in_specs=[pl.BlockSpec(memory_space=pltpu.HBM)] * 2,
        out_specs=(pl.BlockSpec(memory_space=pltpu.VMEM), pl.BlockSpec(memory_space=pltpu.VMEM)),
        scratch_shapes=[
            pltpu.VMEM((GROUP, BANDS, STRIP, TILE), jnp.float32),
            pltpu.VMEM((GROUP, BANDS, STRIP, TILE), jnp.int32),
            pltpu.VMEM((GROUP - 1, STRIP, WIDE), jnp.float32),
            pltpu.VMEM((8, LANES), jnp.float32),
            pltpu.VMEM((8, LANES), jnp.float32),
            pltpu.VMEM((SMALL, 8, LANES), jnp.float32),
            pltpu.VMEM((4, 8, LANES), jnp.float32),
            pltpu.VMEM((2, 8, LANES), jnp.float32),
            pltpu.VMEM((8, LANES), jnp.float32),
            dma((len(GROUPS),)), dma((2,)), dma, dma((4,)),
            pltpu.SemaphoreType.REGULAR((2,)),
        ],
        compiler_params=pltpu.CompilerParams(
            collective_id=0, has_side_effects=True, vmem_limit_bytes=16 * 1024 * 1024),
        name="export",
    )(
        pltpu.with_memory_space_constraint(pixels, pltpu.HBM),
        pltpu.with_memory_space_constraint(valid_flags, pltpu.HBM),
    )
    tile, header = pl.pallas_call(
        place,
        out_shape=shapes,
        in_specs=[pl.BlockSpec(memory_space=pltpu.VMEM)] * 2,
        out_specs=(pl.BlockSpec(memory_space=pltpu.HBM), pl.BlockSpec(memory_space=pltpu.HBM)),
        scratch_shapes=[dma((PARTS + 1,))],
        compiler_params=pltpu.CompilerParams(vmem_limit_bytes=16 * 1024 * 1024),
        name="place",
    )(tile, header)
    return tile.reshape(1, HALF, WIDE), header.T


def solution(mesh):
    placed = (P(None, "dev", None), P(None, "dev", None))
    return jax.shard_map(
        on_device, mesh=mesh, in_specs=placed, out_specs=(P("dev", None, None), P()), check_vma=False
    )
```
